32 devices in a mesh: mem: 4 (over y, x), cell: 8 (over z, core).
Axes of the slice: x: 2, y: 2, z: 4, core: 2. Of those that a mesh axis runs over, the one named last changes fastest.
Arguments:
- state: bfloat16 [16384, 40, 120], P('cell', 'mem'), may hold values from -6 to 6
- vertical_weight: bfloat16 [8192, 120], P('cell'), may hold values from -0.5 to 0.5
- horizontal_weight: float32 [8192, 4], P('cell'), may hold values from 0.05 to 0.45
- obs_slot: int32 [8192, 4], P('cell'), may hold values from 0 to 4095, as said below
- request_cell: int32 [8, 4096], P('cell'), may hold values from 0 to 2047
- obs_value: float32 [8192], P('cell'), may hold values from -6 to 6
- obs_error: float32 [8192], P('cell'), may hold values from 0.5 to 2
- obs_region: int32 [8192], P('cell'), may hold values from 0 to 63, as said below
Outputs:
- cov_matrix: float32 [64, 40, 40], P('cell', 'mem')
- innovation_proj: float32 [64, 40], P('cell', 'mem')
The draws below stay inside these ranges and needn't reach their ends.
Inputs may be any that keep to these rules, and one draw needn't show every extreme that they name: `obs_slot`: within one owner's 1024 observations all 4096 slots differ, so every slot is used: 1024 ask the owner's own patch and 768 each of the four patches at distance 1 and 2. `obs_region`: an observation's region is one of the 8 regions of its owner's patch or of the patches just before or after it (indices wrap); patch p holds regions p * 8 to p * 8 + 7.
All inputs are finite; a program needn't handle non-finite values.
Results may differ from the reference program's by a relative error of at most 0.0003.
Values may be sent and summed in bfloat16 or wider, within the bound.
A program may use at most 128 MiB of HBM per device.

```python
import math
import jax
import jax.numpy as jnp
from jax import lax

MEMBERS = 40
LEV = 120
NEIGH = 4
CELL_DEV = 2048
OBS_DEV = 1024
REG_DEV = 8
HALO_CAP = 768
OWN_CAP = 1024
CELLS = 16384
OBS = 8192
REGIONS = 64
N_CELL = 8


def routing(key):
    base = jax.random.fold_in(key, 71)

    def one_owner(owner_key):
        key_perm, key_cell = jax.random.split(owner_key, 2)
        total = 4 * OBS_DEV
        chosen = jax.random.permutation(key_perm, total).astype(jnp.int32).reshape(OBS_DEV, NEIGH)
        cells = jax.random.randint(key_cell, (total,), 0, CELL_DEV).astype(jnp.int32)
        return (chosen, cells)
    keys = jax.random.split(base, N_CELL)
    chosen, cells = jax.vmap(one_owner)(keys)
    return (chosen.reshape(OBS, NEIGH), cells.reshape(N_CELL, 4 * OBS_DEV))


def draw_obs_slot(key, part):
    return routing(key)[0]


def draw_request_cell(key, part):
    return routing(key)[1]


def draw_obs_region(key, part):
    key_side, key_within = jax.random.split(jax.random.fold_in(key, 53), 2)
    code = jax.random.randint(key_side, (N_CELL, OBS_DEV), 0, 4).astype(jnp.int32)
    moves = jnp.array([-1, 0, 0, 1], dtype=jnp.int32)[code]
    owner = jnp.arange(N_CELL, dtype=jnp.int32)[:, None]
    patch = jnp.mod(owner + moves, N_CELL).astype(jnp.int32)
    within = jax.random.randint(key_within, (N_CELL, OBS_DEV), 0, REG_DEV).astype(jnp.int32)
    return (patch * REG_DEV + within).reshape(OBS).astype(jnp.int32)


def block_scale(rng, shape, shards, least, top_value):
    def one(position, parts):
        heights = jax.random.uniform(jax.random.fold_in(jax.random.fold_in(rng, 6), position), (parts,), jnp.float32, least / len(shards), top_value / len(shards))
        return jnp.repeat(jnp.exp(heights), shape[position] // parts).reshape((-1,) + (1,) * (len(shape) - position - 1))

    factor_of = one(*shards[0])
    for cut in shards[1:]:
        factor_of = factor_of * one(*cut)
    return factor_of


def bell_draw(rng, shape, scale, most, shards=(), held_as=jnp.bfloat16):
    loudness = block_scale(rng, shape, shards, -0.22, 0.18) if shards else 1.0
    values = jax.random.normal(rng, shape, jnp.float32) * scale * loudness
    return jnp.minimum(jnp.maximum(values, -most), most).astype(held_as)


def setup_inputs(seed: int = 0) -> dict:
    key_list = jax.random.split(jax.random.key(seed), 9)
    return {
        "state": bell_draw(key_list[0], (CELLS, MEMBERS, LEV), 1.0, 6.0, ((0, 8), (1, 4))),
        "vertical_weight": bell_draw(key_list[1], (OBS, LEV), LEV ** -0.5, 0.5, ((0, 8),)),
        "horizontal_weight": jnp.clip(0.05 + 0.39999999 * jax.random.uniform(key_list[2], (OBS, NEIGH), jnp.float32) ** block_scale(key_list[2], (OBS, NEIGH), ((0, 8),), -0.2, 0.2), 0.05, 0.45),
        "obs_slot": draw_obs_slot(jax.random.fold_in(key_list[8], 71), 0),
        "request_cell": draw_request_cell(jax.random.fold_in(key_list[8], 71), 0),
        "obs_value": bell_draw(key_list[5], (OBS,), 1.0, 6.0, ((0, 8),), jnp.float32),
        "obs_error": jnp.clip(jnp.exp(math.log(2.0) - 1.3862944 * jax.random.uniform(key_list[6], (OBS,), jnp.float32) ** block_scale(key_list[6], (OBS,), ((0, 8),), -0.2, 0.2)), 0.5, 2.0),
        "obs_region": draw_obs_region(jax.random.fold_in(key_list[8], 71), 0),
    }


def reference(state, vertical_weight, horizontal_weight, obs_slot, request_cell, obs_value, obs_error, obs_region):
    halo_moves = jnp.array([-2, -1, 1, 2], dtype=jnp.int32)

    def block(src):
        slots = lax.dynamic_slice_in_dim(obs_slot, src * OBS_DEV, OBS_DEV, 0)
        table = lax.dynamic_slice_in_dim(request_cell, src, 1, 0)[0]
        within = table[slots]
        which = jnp.minimum(jnp.maximum(slots - OWN_CAP, 0) // HALO_CAP, 3).astype(jnp.int32)
        moved = jnp.mod(src + halo_moves[which], N_CELL).astype(jnp.int32)
        patch = jnp.where(slots < OWN_CAP, src, moved).astype(jnp.int32)
        cells = (patch * CELL_DEV + within).astype(jnp.int32)
        picked = state[cells].astype(jnp.float32)
        levels = lax.dynamic_slice_in_dim(vertical_weight, src * OBS_DEV, OBS_DEV, 0).astype(jnp.float32)
        column = jnp.einsum('okml,ol->okm', picked, levels)
        horiz = lax.dynamic_slice_in_dim(horizontal_weight, src * OBS_DEV, OBS_DEV, 0)
        return jnp.sum(column * horiz[:, :, None], axis=1)

    equiv = lax.map(block, jnp.arange(N_CELL, dtype=jnp.int32)).reshape(OBS, MEMBERS)
    mean = jnp.mean(equiv, axis=1, keepdims=True)
    spread = equiv - mean
    inverse = 1.0 / (obs_error * obs_error)
    innov = (obs_value - mean[:, 0]) * inverse

    def accumulate(carry, src):
        part = lax.dynamic_slice_in_dim(spread, src * OBS_DEV, OBS_DEV, 0)
        scale = lax.dynamic_slice_in_dim(inverse, src * OBS_DEV, OBS_DEV, 0)
        drive = lax.dynamic_slice_in_dim(innov, src * OBS_DEV, OBS_DEV, 0)
        region = lax.dynamic_slice_in_dim(obs_region, src * OBS_DEV, OBS_DEV, 0)
        outer = part[:, :, None] * part[:, None, :] * scale[:, None, None]
        vector = part * drive[:, None]
        total_cov = carry[0] + jax.ops.segment_sum(outer, region, num_segments=REGIONS)
        total_vec = carry[1] + jax.ops.segment_sum(vector, region, num_segments=REGIONS)
        return (total_cov, total_vec), None

    start = (jnp.zeros((REGIONS, MEMBERS, MEMBERS), jnp.float32), jnp.zeros((REGIONS, MEMBERS), jnp.float32))
    result, unused = lax.scan(accumulate, start, jnp.arange(N_CELL, dtype=jnp.int32))
    return result[0], result[1]
```

```python
import functools

import jax
import jax.numpy as jnp
from jax import lax
from jax.experimental import pallas as pl
from jax.experimental.pallas import tpu as pltpu
from jax.sharding import PartitionSpec as P

REG_DEV = 8
TILE = 256
MOVES = (-2, -1, 1, 2)
TERMS = 6
MESH = pl.DeviceIdType.MESH
VMEM = pl.BlockSpec(memory_space=pltpu.VMEM)
NT = (((1,), (1,)), ((), ()))
f32, bf16, i32 = jnp.float32, jnp.bfloat16, jnp.int32


def split(x):
    top = x.astype(bf16).astype(f32)
    return top, x - top


def row16(row):
    return jnp.broadcast_to(row, (16, row.shape[1])).astype(bf16)


def onehot(row, count):
    lanes = row.shape[1]
    ids = lax.broadcasted_iota(i32, (count, lanes), 0).astype(f32).astype(bf16)
    hit = ids.reshape(count // 16, 16, lanes) == row16(row)[None]
    return jnp.where(hit, bf16(1), bf16(0)).reshape(count, lanes)


def spread_rows(row, value, count):
    ids = lax.broadcasted_iota(i32, (count, row.shape[1]), 0).astype(f32)
    return jnp.where(ids == row, value, 0.0)


def ring(axis, by):
    return lax.rem(lax.axis_index(axis) + by + lax.axis_size(axis), lax.axis_size(axis))


def remote(src, dst, send, recv, axis, target):
    return pltpu.make_async_remote_copy(
        src_ref=src,
        dst_ref=dst,
        send_sem=send,
        recv_sem=recv,
        device_id={axis: target},
        device_id_type=MESH,
    )


def segments(own, halo):
    return [(own + h * halo, own + (h + 1) * halo) for h in range(len(MOVES))]


def exchange_kernel(
    own,
    halo,
    table_ref,
    slot_ref,
    h_ref,
    w_ref,
    sorted_ref,
    wall_ref,
    cells,
    sent,
    got,
    send_sem,
    recv_sem,
):
    chunks = own + len(MOVES) * halo
    obs_dev = w_ref.shape[1]
    blocks = obs_dev // TILE
    barrier = pltpu.get_barrier_semaphore()
    for by in MOVES:
        pl.semaphore_signal(
            barrier, inc=1, device_id={"cell": ring("cell", by)}, device_id_type=MESH
        )
    pl.semaphore_wait(barrier, len(MOVES))
    spans = segments(own, halo)
    first, heavy, second = [], [], []
    for h, by in enumerate(MOVES):
        lo, hi = spans[h]
        copy = remote(
            table_ref.at[lo:hi],
            cells.at[lo:hi],
            send_sem.at[h],
            recv_sem.at[h],
            "cell",
            ring("cell", by),
        )
        copy.start()
        first.append(copy)
    for h, by in enumerate(MOVES):
        copy = remote(
            w_ref,
            wall_ref.at[:, (h + 1) * obs_dev : (h + 2) * obs_dev],
            send_sem.at[4 + h],
            recv_sem.at[4 + h],
            "cell",
            ring("cell", by),
        )
        copy.start()
        heavy.append(copy)
    wall_ref[:, :obs_dev] = w_ref[...]

    lane = lax.broadcasted_iota(i32, (1, TILE), 1).astype(f32)
    by_slot = jnp.zeros((4 * chunks, TILE), f32)
    for k in range(slot_ref.shape[0]):
        for j in range(blocks):
            where = slot_ref[k : k + 1, j * TILE : (j + 1) * TILE]
            tops, rest = split(h_ref[k : k + 1, j * TILE : (j + 1) * TILE])
            high = (where >> 8).astype(f32)
            terms = [jnp.full((1, TILE), float(j), f32), lane, tops, rest]
            left = jnp.concatenate([spread_rows(high, t, chunks) for t in terms], axis=0)
            by_slot += lax.dot_general(
                left.astype(bf16),
                onehot((where & 255).astype(f32), TILE),
                NT,
                preferred_element_type=f32,
            )
    slot_obs = by_slot[:chunks] * TILE + by_slot[chunks : 2 * chunks]
    slot_h = by_slot[2 * chunks : 3 * chunks] + by_slot[3 * chunks :]
    for c in range(own, chunks):
        sent[0, c] = slot_obs[c : c + 1]
        sent[1, c] = slot_h[c : c + 1]
    for h, by in enumerate(MOVES):
        lo, hi = spans[h]
        copy = remote(
            sent.at[:, lo:hi],
            got.at[:, lo:hi],
            send_sem.at[8 + h],
            recv_sem.at[8 + h],
            "cell",
            ring("cell", by),
        )
        copy.start()
        second.append(copy)

    for copy in first:
        copy.wait()
    cell_rows = [table_ref[c] if c < own else cells[c] for c in range(chunks)]
    bucket_ids = lax.broadcasted_iota(i32, (8, TILE), 0)
    member_of = jnp.concatenate(
        [jnp.where(bucket_ids == (row >> 8), 1.0, 0.0) for row in cell_rows], axis=0
    )
    rows = 8 * chunks
    place = lax.broadcasted_iota(i32, (TILE, TILE), 0) < lax.broadcasted_iota(i32, (TILE, TILE), 1)
    within = jnp.dot(
        member_of.astype(bf16), jnp.where(place, 1.0, 0.0).astype(bf16), preferred_element_type=f32
    )

    def order(axis):
        index = lax.broadcasted_iota(i32, (rows, rows), axis)
        chunk = index >> 3
        late = jnp.where(chunk >= own + halo, 1, 0)
        return (late * 8 + (index & 7)) * chunks + chunk

    before = jnp.where(order(1) < order(0), 1.0, 0.0).astype(bf16)
    ahead = jnp.dot(before, member_of.astype(bf16), preferred_element_type=f32)
    base = jnp.sum(ahead, axis=1, keepdims=True)
    position = jnp.sum(((within + base) * member_of).reshape(chunks, 8, TILE), axis=1)
    position = position.astype(i32)

    for copy in second:
        copy.wait()
    total = jnp.zeros((TERMS * chunks, TILE), f32)
    for c in range(chunks):
        where = position[c : c + 1]
        cell = cell_rows[c]
        if c < own:
            source, obs, weight = 0, slot_obs[c : c + 1], slot_h[c : c + 1]
        else:
            source, obs, weight = 1 + (c - own) // halo, got[0, c], got[1, c]
        obs = obs.astype(i32)
        tops, rest = split(weight)
        terms = [
            (cell & 255).astype(f32),
            (cell >> 8).astype(f32),
            ((obs >> 8) + source * blocks).astype(f32),
            (obs & 255).astype(f32),
            tops,
            rest,
        ]
        high = (where >> 8).astype(f32)
        left = jnp.concatenate([spread_rows(high, t, chunks) for t in terms], axis=0)
        total += lax.dot_general(
            left.astype(bf16),
            onehot((where & 255).astype(f32), TILE),
            NT,
            preferred_element_type=f32,
        )
    sorted_ref[...] = total
    for copy in heavy:
        copy.wait()


def gather_kernel(own, halo, members, sorted_ref, wall_ref, state_ref, out_ref, wide, value):
    chunks = own + len(MOVES) * halo
    levels = wall_ref.shape[0]
    obs_dev = wall_ref.shape[1] // (1 + len(MOVES))
    blocks = obs_dev // TILE
    buckets = state_ref.shape[1] // TILE
    groups = [
        (0, own + halo, 0, 2 * blocks),
        (own + halo, chunks, 2 * blocks, (1 + len(MOVES)) * blocks),
    ]

    for first, last, low, high in groups:

        def weigh(t, carry):
            upper = sorted_ref[pl.ds(2 * chunks + t, 1), :]
            lower = sorted_ref[pl.ds(3 * chunks + t, 1), :]
            total = jnp.zeros((levels, TILE), f32)
            for k in range(low, high):
                total += jnp.dot(
                    wall_ref[:, k * TILE : (k + 1) * TILE],
                    onehot(jnp.where(upper == k, lower, -1.0), TILE),
                    preferred_element_type=f32,
                )
            wide[t] = total
            value[t] = jnp.zeros((16, TILE), f32)
            return carry

        lax.fori_loop(first, last, weigh, 0)

    for first, last, low, high in groups:
        bucket_of = sorted_ref[chunks + first : chunks + last, :]
        turns = []
        for b in range(1, buckets):
            count = jnp.sum(jnp.where(bucket_of < b, 1.0, 0.0)).astype(i32)
            turns.append(b + lax.shift_right_logical(jnp.maximum(count - 1, 0), 8))

        def step(i, carry):
            b = i32(0)
            for turn in turns:
                b += jnp.where(i >= turn, 1, 0)
            t = first + i - b
            mine = sorted_ref[pl.ds(chunks + t, 1), :] == b.astype(f32)
            row = jnp.where(mine, sorted_ref[pl.ds(t, 1), :], -1.0)
            columns = jnp.dot(
                state_ref[:, pl.ds(pl.multiple_of(b * TILE, TILE), TILE)],
                onehot(row, TILE),
                preferred_element_type=f32,
            ).reshape(members, levels, TILE)
            dots = jnp.sum(columns * wide[t][None], axis=1)
            weight = (
                sorted_ref[pl.ds(4 * chunks + t, 1), :] + sorted_ref[pl.ds(5 * chunks + t, 1), :]
            )
            value[t, :members] = value[t, :members] + dots * weight
            return carry

        steps = last - first + buckets - 1
        unroll = max(u for u in range(1, 9) if steps % u == 0)
        lax.fori_loop(0, steps, step, 0, unroll=unroll)

    for first, last, low, high in groups:
        total = jnp.zeros(((high - low) * 32, TILE), f32)
        for t in range(first, last):
            upper = sorted_ref[2 * chunks + t : 2 * chunks + t + 1, :]
            lower = sorted_ref[3 * chunks + t : 3 * chunks + t + 1, :]
            tops, rest = split(value[t])
            both = jnp.concatenate([tops, rest], axis=0).astype(bf16)
            left = jnp.concatenate(
                [
                    jnp.where(row16(upper)[:1] == bf16(k), both, bf16(0))
                    for k in range(low, high)
                ],
                axis=0,
            )
            total += lax.dot_general(left, onehot(lower, TILE), NT, preferred_element_type=f32)
        for k in range(low, high):
            at = (k - low) * 32
            piece = total[at : at + 16] + total[at + 16 : at + 32]
            j = k % blocks
            out_ref[k // blocks, :, j * TILE : (j + 1) * TILE] = piece[:members]


def combine_kernel(
    equiv_ref,
    value_ref,
    error_ref,
    region_ref,
    cov_ref,
    proj_ref,
    got,
    mine,
    everyone,
    sums,
    halves,
    send_sem,
    recv_sem,
):
    patches, sharers = lax.axis_size("cell"), lax.axis_size("mem")
    here, member = lax.axis_index("cell"), lax.axis_index("mem")
    barrier = pltpu.get_barrier_semaphore()
    for by in MOVES:
        pl.semaphore_signal(
            barrier, inc=1, device_id={"cell": ring("cell", by)}, device_id_type=MESH
        )
    for by in range(1, sharers):
        pl.semaphore_signal(
            barrier, inc=1, device_id={"mem": ring("mem", by)}, device_id_type=MESH
        )
    pl.semaphore_wait(barrier, len(MOVES) + sharers - 1)
    copies = []
    for h, by in enumerate(MOVES):
        copy = remote(
            equiv_ref.at[1 + h],
            got.at[h],
            send_sem.at[h],
            recv_sem.at[h],
            "cell",
            ring("cell", -by),
        )
        copy.start()
        copies.append(copy)
    error = error_ref[...]
    inverse = 1.0 / (error * error)
    region = region_ref[...] - (here - 1) * REG_DEV
    region = jnp.where(region < 0, region + patches * REG_DEV, region)
    region = jnp.where(region >= patches * REG_DEV, region - patches * REG_DEV, region)
    for copy in copies:
        copy.wait()
    own = equiv_ref[0]
    for h in range(len(MOVES)):
        own = own + got[h]
    mine[...] = own
    copies = []
    for by in range(1, sharers):
        copy = remote(
            mine,
            everyone.at[member],
            send_sem.at[3 + by],
            recv_sem.at[3 + by],
            "mem",
            ring("mem", by),
        )
        copy.start()
        copies.append(copy)
    everyone[member] = own
    for copy in copies:
        copy.wait()
    whole = jnp.concatenate([everyone[s] for s in range(sharers)], axis=0)
    total = whole.shape[0]
    mean = jnp.sum(whole, axis=0, keepdims=True) * (1.0 / total)
    innov = value_ref[...] - mean
    right = jnp.concatenate([whole - mean, innov], axis=0) * inverse
    pad = -right.shape[0] % 16
    right = jnp.concatenate([right, jnp.zeros((pad, right.shape[1]), f32)], axis=0)
    right_top, right_rest = [x.astype(bf16) for x in split(right)]
    spread = own - mean
    count = own.shape[0]
    ids = lax.broadcasted_iota(i32, (REG_DEV, region.shape[1]), 0)
    hits = [ids + part * REG_DEV == region for part in range(3)]
    lefts = []
    for piece in split(spread):
        lefts.append(
            jnp.concatenate(
                [
                    jnp.where(hit, piece[m : m + 1], 0.0)
                    for hit in hits
                    for m in range(count)
                ],
                axis=0,
            ).astype(bf16)
        )
    product = functools.partial(lax.dot_general, dimension_numbers=NT, preferred_element_type=f32)
    result = (
        product(lefts[0], right_top) + product(lefts[0], right_rest) + product(lefts[1], right_top)
    )
    rows = count * REG_DEV
    for part in range(3):
        sums[part] = result[part * rows : (part + 1) * rows]
    copies = []
    for slot, (part, by) in enumerate(((0, -1), (2, 1))):
        copy = remote(
            sums.at[part],
            halves.at[slot],
            send_sem.at[3 + sharers + slot],
            recv_sem.at[3 + sharers + slot],
            "cell",
            ring("cell", by),
        )
        copy.start()
        copies.append(copy)
    for copy in copies:
        copy.wait()
    final = result[rows : 2 * rows] + halves[0] + halves[1]
    final = final.reshape(count, REG_DEV, final.shape[1])
    cov_ref[...] = final[:, :, :total]
    lanes = lax.broadcasted_iota(i32, (REG_DEV, count), 1)
    proj = jnp.zeros((REG_DEV, count), f32)
    for m in range(count):
        proj = jnp.where(lanes == m, final[m, :, total : total + 1], proj)
    proj_ref[...] = proj


def on_device(
    state,
    vertical_weight,
    horizontal_weight,
    obs_slot,
    request_cell,
    obs_value,
    obs_error,
    obs_region,
):
    sharers = lax.axis_size("mem")
    cell_dev, members, levels = state.shape
    obs_dev, neigh = obs_slot.shape
    own = obs_dev // TILE
    halo = 3 * obs_dev // 4 // TILE
    chunks = own + len(MOVES) * halo
    sources = 1 + len(MOVES)
    ordered, wall = pl.pallas_call(
        functools.partial(exchange_kernel, own, halo),
        out_shape=(
            jax.ShapeDtypeStruct((TERMS * chunks, TILE), f32),
            jax.ShapeDtypeStruct((levels, sources * obs_dev), bf16),
        ),
        in_specs=[VMEM] * 4,
        out_specs=(VMEM, VMEM),
        scratch_shapes=[
            pltpu.VMEM((chunks, 1, TILE), i32),
            pltpu.VMEM((2, chunks, 1, TILE), f32),
            pltpu.VMEM((2, chunks, 1, TILE), f32),
            pltpu.SemaphoreType.DMA((12,)),
            pltpu.SemaphoreType.DMA((12,)),
        ],
        compiler_params=pltpu.CompilerParams(
            collective_id=0, has_side_effects=True, vmem_limit_bytes=24 * 2**20
        ),
    )(
        request_cell.reshape(chunks, 1, TILE),
        obs_slot.T,
        horizontal_weight.T,
        vertical_weight.T,
    )
    equiv = pl.pallas_call(
        functools.partial(gather_kernel, own, halo, members),
        out_shape=jax.ShapeDtypeStruct((sources, members, obs_dev), f32),
        in_specs=[VMEM] * 3,
        out_specs=VMEM,
        scratch_shapes=[
            pltpu.VMEM((chunks, levels, TILE), f32),
            pltpu.VMEM((chunks, 16, TILE), f32),
        ],
        compiler_params=pltpu.CompilerParams(vmem_limit_bytes=32 * 2**20),
    )(ordered, wall, state.transpose(1, 2, 0).reshape(members * levels, cell_dev))
    everyone = sharers * members
    width = everyone + 1 + (-(everyone + 1)) % 16
    rows = members * REG_DEV
    cov, proj = pl.pallas_call(
        combine_kernel,
        out_shape=(
            jax.ShapeDtypeStruct((members, REG_DEV, everyone), f32),
            jax.ShapeDtypeStruct((REG_DEV, members), f32),
        ),
        in_specs=[VMEM] * 4,
        out_specs=(VMEM, VMEM),
        scratch_shapes=[
            pltpu.VMEM((len(MOVES), members, obs_dev), f32),
            pltpu.VMEM((members, obs_dev), f32),
            pltpu.VMEM((sharers, members, obs_dev), f32),
            pltpu.VMEM((3, rows, width), f32),
            pltpu.VMEM((2, rows, width), f32),
            pltpu.SemaphoreType.DMA((5 + sharers,)),
            pltpu.SemaphoreType.DMA((5 + sharers,)),
        ],
        compiler_params=pltpu.CompilerParams(
            collective_id=1, has_side_effects=True, vmem_limit_bytes=24 * 2**20
        ),
    )(
        equiv,
        obs_value.reshape(1, obs_dev),
        obs_error.reshape(1, obs_dev),
        obs_region.reshape(1, obs_dev),
    )
    return cov.transpose(1, 0, 2), proj


def solution(mesh):
    in_specs = (
        P("cell", "mem", None),
        P("cell", None),
        P("cell", None),
        P("cell", None),
        P("cell", None),
        P("cell"),
        P("cell"),
        P("cell"),
    )
    out_specs = (P("cell", "mem", None), P("cell", "mem"))
    return jax.shard_map(
        on_device, mesh=mesh, in_specs=in_specs, out_specs=out_specs, check_vma=False
    )
```

```python
import functools

import jax
import jax.numpy as jnp
from jax import lax
from jax.experimental import pallas as pl
from jax.experimental.pallas import tpu as pltpu
from jax.sharding import PartitionSpec as P

REG_DEV = 8
TILE = 256
MOVES = (-2, -1, 1, 2)
ANY = pl.BlockSpec(memory_space=pl.ANY)
MESH = pl.DeviceIdType.MESH
VMEM = pl.BlockSpec(memory_space=pltpu.VMEM)
NT = (((1,), (1,)), ((), ()))
f32, bf16, i32 = jnp.float32, jnp.bfloat16, jnp.int32


def split(x):
    top = x.astype(bf16).astype(f32)
    return top, x - top


def row16(row):
    return jnp.broadcast_to(row, (16, row.shape[1])).astype(bf16)


def onehot(row, count):
    lanes = row.shape[1]
    ids = lax.broadcasted_iota(i32, (count, lanes), 0).astype(f32).astype(bf16)
    hit = ids.reshape(count // 16, 16, lanes) == row16(row)[None]
    return jnp.where(hit, bf16(1), bf16(0)).reshape(count, lanes)


def spread_rows(row, value, count):
    ids = lax.broadcasted_iota(i32, (count, row.shape[1]), 0).astype(f32)
    return jnp.where(ids == row, value, 0.0)


def ring(axis, by):
    return lax.rem(lax.axis_index(axis) + by + lax.axis_size(axis), lax.axis_size(axis))


def remote(src, dst, send, recv, **target):
    return pltpu.make_async_remote_copy(
        src_ref=src,
        dst_ref=dst,
        send_sem=send,
        recv_sem=recv,
        device_id=target,
        device_id_type=MESH,
    )


def started(*args, **target):
    copy = remote(*args, **target)
    copy.start()
    return copy


def spread_sum(wheres, terms_of, count):
    total = None
    for where, terms in zip(wheres, terms_of):
        high = (where >> 8).astype(f32)
        left = jnp.concatenate([spread_rows(high, t, count) for t in terms], axis=0)
        part = lax.dot_general(
            left.astype(bf16),
            onehot((where & 255).astype(f32), TILE),
            NT,
            preferred_element_type=f32,
        )
        total = part if total is None else total + part
    return total


def bucket_at(turns, i):
    b = i32(0)
    for turn in turns:
        b += jnp.where(i >= turn, 1, 0)
    return b


def largest_divisor(n, most):
    return max(u for u in range(1, most + 1) if n % u == 0)


def kernel(
    own,
    halo,
    table_hbm,
    slot_hbm,
    h_hbm,
    w_hbm,
    state_hbm,
    value_hbm,
    error_hbm,
    region_hbm,
    cov_ref,
    proj_ref,
    table_ref,
    slot_ref,
    h_ref,
    wall_ref,
    state_ref,
    value_ref,
    error_ref,
    region_ref,
    cells,
    sent,
    got,
    sorted_ref,
    picked,
    wide,
    dots_ref,
    equiv,
    gathered,
    sums,
    shares,
    load_sem,
    cell_send,
    cell_recv,
    wall_send,
    wall_recv,
    note_send,
    note_recv,
    equiv_send,
    equiv_recv,
    sums_send,
    sums_recv,
):
    far = len(MOVES)
    chunks = own + far * halo
    levels, obs_dev = w_hbm.shape
    members = state_hbm.shape[0] // levels
    blocks = obs_dev // TILE
    buckets = state_hbm.shape[1] // TILE
    patches, sharers = lax.axis_size("cell"), lax.axis_size("mem")
    here, member = lax.axis_index("cell"), lax.axis_index("mem")
    share = obs_dev // sharers

    loads = []
    for number, (src, dst) in enumerate(
        (
            (table_hbm, table_ref),
            (w_hbm, wall_ref.at[:, :obs_dev]),
            (slot_hbm, slot_ref),
            (h_hbm, h_ref),
            (state_hbm, state_ref),
            (value_hbm, value_ref),
            (error_hbm, error_ref),
            (region_hbm, region_ref),
        )
    ):
        copy = pltpu.make_async_copy(src, dst, load_sem.at[number])
        copy.start()
        loads.append(copy)
    barrier = pltpu.get_barrier_semaphore()
    greeted = [(m, c) for m in range(sharers) for c in (0,) + MOVES if (m, c) != (0, 0)]
    for m, c in greeted:
        pl.semaphore_signal(
            barrier,
            inc=1,
            device_id={"mem": ring("mem", m), "cell": ring("cell", c)},
            device_id_type=MESH,
        )

    even = 1 - lax.rem(here, 2)
    outer = 1 - 2 * even
    offsets = (0, -outer, outer, 2 * outer, -2 * outer)
    asked = (0, -outer, outer, -2 * outer, 2 * outer)
    part_of = (0, 1 + even, 2 - even, 3 * even, 3 - 3 * even)
    cell_of = [ring("cell", by) for by in offsets]
    asked_of = [ring("cell", by) for by in asked]

    loads[0].wait()
    loads[1].wait()
    pl.semaphore_wait(barrier, len(greeted))

    def segment(k):
        return pl.ds(own + part_of[k] * halo, halo)

    def landing(k):
        return pl.ds(own + (k - 1) * halo, halo)

    first = [
        started(
            table_ref.at[segment(k)],
            cells.at[landing(k)],
            cell_send.at[k],
            cell_recv.at[k],
            cell=asked_of[k],
        )
        for k in range(1, 1 + far)
    ]
    mine = wall_ref.at[:, :obs_dev]
    heavy = [
        started(
            mine,
            wall_ref.at[:, k * obs_dev : (k + 1) * obs_dev],
            wall_send.at[k],
            wall_recv.at[k],
            cell=asked_of[k],
        )
        for k in range(1, far)
    ]

    loads[2].wait()
    loads[3].wait()
    lane = lax.broadcasted_iota(i32, (1, TILE), 1).astype(f32)
    wheres, terms_of = [], []
    for k in range(slot_ref.shape[0]):
        for j in range(blocks):
            tops, rest = split(h_ref[k : k + 1, j * TILE : (j + 1) * TILE])
            wheres.append(slot_ref[k : k + 1, j * TILE : (j + 1) * TILE])
            terms_of.append([jnp.full((1, TILE), float(j), f32), lane, tops, rest])
    by_slot = spread_sum(wheres, terms_of, chunks)
    slot_obs = by_slot[:chunks] * TILE + by_slot[chunks : 2 * chunks]
    slot_h = by_slot[2 * chunks : 3 * chunks] + by_slot[3 * chunks :]
    for c in range(chunks):
        sent[0, c] = slot_obs[c : c + 1]
        sent[1, c] = slot_h[c : c + 1]
    second = [
        started(
            sent.at[:, segment(k)],
            got.at[:, landing(k)],
            note_send.at[k],
            note_recv.at[k],
            cell=asked_of[k],
        )
        for k in range(1, 1 + far)
    ]

    for copy in first:
        copy.wait()
    cell_rows = [table_ref[c] if c < own else cells[c] for c in range(chunks)]
    bucket_ids = lax.broadcasted_iota(i32, (8, TILE), 0)
    member_of = jnp.concatenate(
        [jnp.where(bucket_ids == (row >> 8), 1.0, 0.0) for row in cell_rows], axis=0
    )
    rows = 8 * chunks
    place = lax.broadcasted_iota(i32, (TILE, TILE), 0) < lax.broadcasted_iota(i32, (TILE, TILE), 1)
    within = jnp.dot(
        member_of.astype(bf16), jnp.where(place, 1.0, 0.0).astype(bf16), preferred_element_type=f32
    )

    def order(axis):
        index = lax.broadcasted_iota(i32, (rows, rows), axis)
        chunk = index >> 3
        late = jnp.where(chunk >= own + halo, 1, 0)
        return (late * 8 + (index & 7)) * chunks + chunk

    before = jnp.where(order(1) < order(0), 1.0, 0.0).astype(bf16)
    ahead = jnp.dot(before, member_of.astype(bf16), preferred_element_type=f32)
    base = jnp.sum(ahead, axis=1, keepdims=True)
    position = jnp.sum(((within + base) * member_of).reshape(chunks, 8, TILE), axis=1)
    position = position.astype(i32)
    wheres = [position[c : c + 1] for c in range(chunks)]
    sorted_ref[: 2 * chunks] = spread_sum(
        wheres, [[(c & 255).astype(f32), (c >> 8).astype(f32)] for c in cell_rows], chunks
    )

    groups = [
        (0, own + halo, 0, 2 * blocks),
        (own + halo, chunks, 2 * blocks, (1 + far) * blocks),
    ]
    turns_of, starts, at = [], [], 0
    for low, high, _, _ in groups:
        turns = []
        for b in range(1, buckets):
            below = sum(jnp.where(row < b * TILE, 1, 0) for row in cell_rows[low:high])
            count = jnp.sum(below)
            turns.append(b + lax.shift_right_logical(jnp.maximum(count - 1, 0), 8))
        turns_of.append(turns)
        starts.append(at)
        at += high - low + buckets - 1
    loads[4].wait()
    for (low, high, _, _), turns, start in zip(groups, turns_of, starts):

        def pick(i, carry):
            b = bucket_at(turns, i)
            t = low + i - b
            held = sorted_ref[pl.ds(chunks + t, 1), :] == b.astype(f32)
            row = jnp.where(held, sorted_ref[pl.ds(t, 1), :], -1.0)
            picked[start + i] = jnp.dot(
                state_ref[:, pl.ds(b * TILE, TILE)],
                onehot(row, TILE),
                preferred_element_type=f32,
            )
            return carry

        steps = high - low + buckets - 1
        lax.fori_loop(0, steps, pick, 0, unroll=largest_divisor(steps, 8))

    for copy in second:
        copy.wait()
    terms_of = []
    for c in range(chunks):
        if c < own:
            source, obs, weight = 0, slot_obs[c : c + 1], slot_h[c : c + 1]
        else:
            source, obs, weight = 1 + (c - own) // halo, got[0, c], got[1, c]
        obs = obs.astype(i32)
        upper = ((obs >> 8) + source * blocks).astype(f32)
        terms_of.append([upper, (obs & 255).astype(f32), *split(weight)])
    sorted_ref[2 * chunks :] = spread_sum(wheres, terms_of, chunks)

    forward = None
    replies = []
    for number, ((low, high, near, end), turns, start) in enumerate(
        zip(groups, turns_of, starts)
    ):
        if number == 0:
            heavy[0].wait()
        else:
            heavy[1].wait()
            forward = started(
                wall_ref.at[:, 2 * obs_dev : 3 * obs_dev],
                wall_ref.at[:, 4 * obs_dev :],
                wall_send.at[4],
                wall_recv.at[4],
                cell=cell_of[1],
            )
            heavy[2].wait()
            forward.wait()

        def weigh(t, carry):
            upper = sorted_ref[pl.ds(2 * chunks + t, 1), :]
            lower = sorted_ref[pl.ds(3 * chunks + t, 1), :]
            total = jnp.zeros((levels, TILE), f32)
            for k in range(near, end):
                total += jnp.dot(
                    wall_ref[:, k * TILE : (k + 1) * TILE],
                    onehot(jnp.where(upper == k, lower, -1.0), TILE),
                    preferred_element_type=f32,
                )
            wide[t] = total
            return carry

        lax.fori_loop(low, high, weigh, 0, unroll=largest_divisor(high - low, 7))

        def reduce(i, carry):
            t = low + i - bucket_at(turns, i)
            columns = picked[start + i].reshape(members, levels, TILE)
            dots_ref[start + i, :members] = jnp.sum(columns * wide[t][None], axis=1)
            return carry

        steps = high - low + buckets - 1
        lax.fori_loop(0, steps, reduce, 0, unroll=largest_divisor(steps, 2))

        total = jnp.zeros(((end - near) * 32, TILE), f32)
        for t in range(low, high):
            upper = sorted_ref[2 * chunks + t : 2 * chunks + t + 1, :]
            lower = sorted_ref[3 * chunks + t : 3 * chunks + t + 1, :]
            weight = (
                sorted_ref[4 * chunks + t : 4 * chunks + t + 1, :]
                + sorted_ref[5 * chunks + t : 5 * chunks + t + 1, :]
            )
            dots = jnp.zeros((members, TILE), f32)
            for b in range(buckets):
                at = t - low + b
                here_b = (bucket_at(turns, at) == b).astype(i32).astype(f32)
                dots += here_b * dots_ref[start + at, :members]
            dots = jnp.concatenate(
                [dots * weight, jnp.zeros((16 - members, TILE), f32)], axis=0
            )
            both = jnp.concatenate(split(dots), axis=0).astype(bf16)
            key = row16(upper)[:1]
            left = jnp.concatenate(
                [jnp.where(key == bf16(k), both, bf16(0)) for k in range(near, end)], axis=0
            )
            total += lax.dot_general(left, onehot(lower, TILE), NT, preferred_element_type=f32)
        for k in range(near, end):
            at = (k - near) * 32
            piece = total[at : at + 16] + total[at + 16 : at + 32]
            source, lanes = k // blocks, k % blocks * TILE
            equiv[source, lanes // share, :, lanes % share : lanes % share + TILE] = piece[
                :members
            ]
        for source in range(near // blocks, end // blocks):
            for by in range(sharers):
                if source or by:
                    target = ring("mem", by)
                    replies.append(
                        started(
                            equiv.at[source, target],
                            gathered.at[source, member],
                            equiv_send.at[source * sharers + by],
                            equiv_recv.at[source * sharers + by],
                            mem=target,
                            cell=cell_of[source],
                        )
                    )

    for load in loads[5:]:
        load.wait()
    lanes = pl.ds(pl.multiple_of(member * share, 128), share)
    error = error_ref[:, lanes]
    inverse = 1.0 / (error * error)
    region = region_ref[:, lanes] - (here - 1) * REG_DEV
    region = jnp.where(region < 0, region + patches * REG_DEV, region)
    region = jnp.where(region >= patches * REG_DEV, region - patches * REG_DEV, region)
    gathered[0, member] = equiv[0, member]
    for copy in replies:
        copy.wait()
    whole = []
    for m in range(sharers):
        piece = gathered[0, m]
        for source in range(1, 1 + far):
            piece = piece + gathered[source, m]
        whole.append(piece)
    whole = jnp.concatenate(whole, axis=0)
    everyone = whole.shape[0]
    mean = jnp.sum(whole, axis=0, keepdims=True) * (1.0 / everyone)
    spread = whole - mean
    innov = value_ref[:, lanes] - mean
    right = jnp.concatenate([spread, innov], axis=0) * inverse
    width = sums.shape[-1] // 2
    blank = jnp.zeros((width - everyone - 1, share), f32)
    right = [jnp.concatenate([x, blank], axis=0) for x in split(right)]
    zero = jnp.zeros((width, share), f32)
    ids = lax.broadcasted_iota(i32, (REG_DEV, share), 0)
    hits = [ids + part * REG_DEV == region for part in range(3)]
    product = functools.partial(lax.dot_general, dimension_numbers=NT, preferred_element_type=f32)
    half = members // 2
    result = None
    for side in range(2):
        rights = [
            jnp.concatenate([x, zero] if side == 0 else [zero, x], axis=0).astype(bf16)
            for x in right
        ]
        lefts = []
        for piece in split(spread):
            lefts.append(
                jnp.concatenate(
                    [
                        jnp.where(hit, piece[at : at + 1], 0.0)
                        for m in range(sharers)
                        for hit in hits
                        for at in range(m * members + side * half, m * members + (side + 1) * half)
                    ],
                    axis=0,
                ).astype(bf16)
            )
        part = (
            product(lefts[0], rights[0])
            + product(lefts[0], rights[1])
            + product(lefts[1], rights[0])
        )
        result = part if result is None else result + part
    sums[...] = result.reshape(sums.shape)
    copies = []
    for by in range(sharers):
        target = ring("mem", by)
        for part in range(3):
            if by or part != 1:
                number = by * 3 + part
                copies.append(
                    started(
                        sums.at[target, part],
                        shares.at[member, part],
                        sums_send.at[number],
                        sums_recv.at[number],
                        mem=target,
                        cell=ring("cell", part - 1),
                    )
                )
    shares[member, 1] = sums[member, 1]
    for copy in copies:
        copy.wait()
    final = shares[0, 0]
    for m in range(sharers):
        for part in range(3):
            if m or part:
                final = final + shares[m, part]
    final = final.reshape(half, REG_DEV, 2 * width)
    cov_ref[:half] = final[:, :, :everyone]
    cov_ref[half:] = final[:, :, width : width + everyone]
    lanes = lax.broadcasted_iota(i32, (REG_DEV, members), 1)
    proj = jnp.zeros((REG_DEV, members), f32)
    for m in range(members):
        at = everyone + m // half * width
        proj = jnp.where(lanes == m, final[m % half, :, at : at + 1], proj)
    proj_ref[...] = proj


def on_device(
    state,
    vertical_weight,
    horizontal_weight,
    obs_slot,
    request_cell,
    obs_value,
    obs_error,
    obs_region,
):
    sharers = lax.axis_size("mem")
    cell_dev, members, levels = state.shape
    obs_dev, neigh = obs_slot.shape
    own = obs_dev // TILE
    halo = 3 * obs_dev // 4 // TILE
    far = len(MOVES)
    chunks = own + far * halo
    sources = 1 + far
    buckets = cell_dev // TILE
    steps = chunks + 2 * (buckets - 1)
    share = obs_dev // sharers
    everyone = sharers * members
    width = everyone + 1 + (-(everyone + 1)) % 16
    rows = members // 2 * REG_DEV
    dma = lambda n: pltpu.SemaphoreType.DMA((n,))
    cov, proj = pl.pallas_call(
        functools.partial(kernel, own, halo),
        out_shape=(
            jax.ShapeDtypeStruct((members, REG_DEV, everyone), f32),
            jax.ShapeDtypeStruct((REG_DEV, members), f32),
        ),
        in_specs=[ANY] * 8,
        out_specs=(VMEM, VMEM),
        scratch_shapes=[
            pltpu.VMEM((chunks, 1, TILE), i32),
            pltpu.VMEM((neigh, obs_dev), i32),
            pltpu.VMEM((neigh, obs_dev), f32),
            pltpu.VMEM((levels, sources * obs_dev), bf16),
            pltpu.VMEM((members * levels, cell_dev), bf16),
            pltpu.VMEM((1, obs_dev), f32),
            pltpu.VMEM((1, obs_dev), f32),
            pltpu.VMEM((1, obs_dev), i32),
            pltpu.VMEM((chunks, 1, TILE), i32),
            pltpu.VMEM((2, chunks, 1, TILE), f32),
            pltpu.VMEM((2, chunks, 1, TILE), f32),
            pltpu.VMEM((6 * chunks, TILE), f32),
            pltpu.VMEM((steps, members * levels, TILE), f32),
            pltpu.VMEM((chunks, levels, TILE), f32),
            pltpu.VMEM((steps, 16, TILE), f32),
            pltpu.VMEM((sources, sharers, members, share), f32),
            pltpu.VMEM((sources, sharers, members, share), f32),
            pltpu.VMEM((sharers, 3, rows, 2 * width), f32),
            pltpu.VMEM((sharers, 3, rows, 2 * width), f32),
            dma(8),
            dma(5),
            dma(5),
            dma(5),
            dma(5),
            dma(5),
            dma(5),
            dma(sources * sharers),
            dma(sources * sharers),
            dma(3 * sharers),
            dma(3 * sharers),
        ],
        compiler_params=pltpu.CompilerParams(
            collective_id=0, has_side_effects=True, vmem_limit_bytes=63 * 2**20
        ),
    )(
        request_cell.reshape(chunks, 1, TILE),
        obs_slot.T,
        horizontal_weight.T,
        vertical_weight.T,
        state.transpose(1, 2, 0).reshape(members * levels, cell_dev),
        obs_value.reshape(1, obs_dev),
        obs_error.reshape(1, obs_dev),
        obs_region.reshape(1, obs_dev),
    )
    return cov.transpose(1, 0, 2), proj


def solution(mesh):
    in_specs = (
        P("cell", "mem", None),
        P("cell", None),
        P("cell", None),
        P("cell", None),
        P("cell", None),
        P("cell"),
        P("cell"),
        P("cell"),
    )
    out_specs = (P("cell", "mem", None), P("cell", "mem"))
    return jax.shard_map(
        on_device, mesh=mesh, in_specs=in_specs, out_specs=out_specs, check_vma=False
    )
```

```python
import functools

import jax
import jax.numpy as jnp
from jax import lax
from jax.experimental import pallas as pl
from jax.experimental.pallas import tpu as pltpu
from jax.sharding import PartitionSpec as P

REG_DEV = 8
TILE = 256
MOVES = (-2, -1, 1, 2)
HBM = pl.BlockSpec(memory_space=pltpu.HBM)
MESH = pl.DeviceIdType.MESH
VMEM = pl.BlockSpec(memory_space=pltpu.VMEM)
NT = (((1,), (1,)), ((), ()))
f32, bf16, i32 = jnp.float32, jnp.bfloat16, jnp.int32


def split(x):
    top = x.astype(bf16).astype(f32)
    return top, x - top


def row16(row):
    return jnp.broadcast_to(row, (16, row.shape[1])).astype(bf16)


def onehot(row, count):
    lanes = row.shape[1]
    ids = lax.broadcasted_iota(i32, (count, lanes), 0).astype(f32).astype(bf16)
    hit = ids.reshape(count // 16, 16, lanes) == row16(row)[None]
    return jnp.where(hit, bf16(1), bf16(0)).reshape(count, lanes)


def spread_rows(row, value, count):
    ids = lax.broadcasted_iota(i32, (count, row.shape[1]), 0).astype(f32)
    return jnp.where(ids == row, value, 0.0)


def ring(axis, by):
    return lax.rem(lax.axis_index(axis) + by + lax.axis_size(axis), lax.axis_size(axis))


def remote(src, dst, send, recv, **target):
    return pltpu.make_async_remote_copy(
        src_ref=src,
        dst_ref=dst,
        send_sem=send,
        recv_sem=recv,
        device_id=target,
        device_id_type=MESH,
    )


def started(*args, **target):
    copy = remote(*args, **target)
    copy.start()
    return copy


def spread_sum(wheres, terms_of, count):
    total = None
    for where, terms in zip(wheres, terms_of):
        high = (where >> 8).astype(f32)
        left = jnp.concatenate([spread_rows(high, t, count) for t in terms], axis=0)
        part = lax.dot_general(
            left.astype(bf16),
            onehot((where & 255).astype(f32), TILE),
            NT,
            preferred_element_type=f32,
        )
        total = part if total is None else total + part
    return total


def bucket_at(turns, i):
    b = i32(0)
    for turn in turns:
        b += jnp.where(i >= turn, 1, 0)
    return b


def largest_divisor(n, most):
    return max(u for u in range(1, most + 1) if n % u == 0)


def kernel(
    own,
    halo,
    table_hbm,
    slot_hbm,
    h_hbm,
    w_hbm,
    state_hbm,
    value_hbm,
    error_hbm,
    region_hbm,
    out_ref,
    table_ref,
    slot_ref,
    h_ref,
    wall_ref,
    state_ref,
    value_ref,
    error_ref,
    region_ref,
    cells,
    sent,
    got,
    sorted_ref,
    wide,
    dots_ref,
    equiv,
    gathered,
    sums,
    shares,
    load_sem,
    cell_send,
    cell_recv,
    wall_send,
    wall_recv,
    pass_send,
    pass_recv,
    note_send,
    note_recv,
    equiv_send,
    equiv_recv,
    sums_send,
    sums_recv,
):
    far = len(MOVES)
    chunks = own + far * halo
    levels, obs_dev = w_hbm.shape
    members = state_hbm.shape[0] // levels
    blocks = obs_dev // TILE
    buckets = state_hbm.shape[1] // TILE
    patches, sharers = lax.axis_size("cell"), lax.axis_size("mem")
    here, member = lax.axis_index("cell"), lax.axis_index("mem")
    share = obs_dev // sharers

    loads = []
    for number, (src, dst) in enumerate(
        (
            (table_hbm, table_ref),
            (w_hbm, wall_ref.at[:, :obs_dev]),
            (slot_hbm, slot_ref),
            (h_hbm, h_ref),
            (state_hbm, state_ref),
            (value_hbm, value_ref),
            (error_hbm, error_ref),
            (region_hbm, region_ref),
        )
    ):
        copy = pltpu.make_async_copy(src, dst, load_sem.at[number])
        copy.start()
        loads.append(copy)
    barrier = pltpu.get_barrier_semaphore()
    greeted = [(m, c) for m in range(sharers) for c in (0,) + MOVES if (m, c) != (0, 0)]
    for m, c in greeted:
        pl.semaphore_signal(
            barrier,
            inc=1,
            device_id={"mem": ring("mem", m), "cell": ring("cell", c)},
            device_id_type=MESH,
        )

    even = 1 - lax.rem(here, 2)
    outer = 1 - 2 * even
    offsets = (0, -outer, outer, 2 * outer, -2 * outer)
    asked = (0, -outer, outer, -2 * outer, 2 * outer)
    part_of = (0, 1 + even, 2 - even, 3 * even, 3 - 3 * even)
    cell_of = [ring("cell", by) for by in offsets]
    asked_of = [ring("cell", by) for by in asked]

    loads[2].wait()
    loads[3].wait()
    lane = lax.broadcasted_iota(i32, (1, TILE), 1).astype(f32)
    wheres, terms_of = [], []
    for k in range(slot_ref.shape[0]):
        for j in range(blocks):
            tops, rest = split(h_ref[k : k + 1, j * TILE : (j + 1) * TILE])
            wheres.append(slot_ref[k : k + 1, j * TILE : (j + 1) * TILE])
            terms_of.append([jnp.full((1, TILE), float(j), f32), lane, tops, rest])
    by_slot = spread_sum(wheres, terms_of, chunks)
    slot_obs = by_slot[:chunks] * TILE + by_slot[chunks : 2 * chunks]
    slot_h = by_slot[2 * chunks : 3 * chunks] + by_slot[3 * chunks :]
    for c in range(chunks):
        sent[0, c] = slot_obs[c : c + 1]
        sent[1, c] = slot_h[c : c + 1]
    loads[0].wait()
    loads[1].wait()
    pl.semaphore_wait(barrier, len(greeted))

    def segment(k):
        return pl.ds(own + part_of[k] * halo, halo)

    def landing(k):
        return pl.ds(own + (k - 1) * halo, halo)

    first = [
        started(
            table_ref.at[segment(k)],
            cells.at[landing(k)],
            cell_send.at[k],
            cell_recv.at[k],
            cell=asked_of[k],
        )
        for k in range(1, 1 + far)
    ]
    second = [
        started(
            sent.at[:, segment(k)],
            got.at[:, landing(k)],
            note_send.at[k],
            note_recv.at[k],
            cell=asked_of[k],
        )
        for k in range(1, 1 + far)
    ]

    def quarter(k):
        return wall_ref.at[:, pl.ds(pl.multiple_of(k * obs_dev + member * share, 128), share)]

    def whole_wall(k):
        return wall_ref.at[:, k * obs_dev : (k + 1) * obs_dev]

    outward = started(
        quarter(0), quarter(2), wall_send.at[2], wall_recv.at[2], cell=asked_of[2]
    )
    near_wall = started(
        whole_wall(0), whole_wall(1), wall_send.at[1], wall_recv.at[1], cell=asked_of[1]
    )
    inward = started(
        whole_wall(0), whole_wall(3), wall_send.at[3], wall_recv.at[3], cell=asked_of[3]
    )

    for copy in first:
        copy.wait()
    cell_rows = [table_ref[c] if c < own else cells[c] for c in range(chunks)]
    bucket_ids = lax.broadcasted_iota(i32, (8, TILE), 0)
    member_of = jnp.concatenate(
        [jnp.where(bucket_ids == (row >> 8), 1.0, 0.0) for row in cell_rows], axis=0
    )
    rows = 8 * chunks
    place = lax.broadcasted_iota(i32, (TILE, TILE), 0) < lax.broadcasted_iota(i32, (TILE, TILE), 1)
    within = jnp.dot(
        member_of.astype(bf16), jnp.where(place, 1.0, 0.0).astype(bf16), preferred_element_type=f32
    )

    def order(axis):
        index = lax.broadcasted_iota(i32, (rows, rows), axis)
        chunk = index >> 3
        late = jnp.where(chunk >= own + halo, 1, 0)
        return (late * 8 + (index & 7)) * chunks + chunk

    before = jnp.where(order(1) < order(0), 1.0, 0.0).astype(bf16)
    ahead = jnp.dot(before, member_of.astype(bf16), preferred_element_type=f32)
    base = jnp.sum(ahead, axis=1, keepdims=True)
    position = jnp.sum(((within + base) * member_of).reshape(chunks, 8, TILE), axis=1)
    position = position.astype(i32)
    for copy in second:
        copy.wait()
    terms_of = []
    for c, cell in enumerate(cell_rows):
        if c < own:
            source, obs, weight = 0, slot_obs[c : c + 1], slot_h[c : c + 1]
        else:
            source, obs, weight = 1 + (c - own) // halo, got[0, c], got[1, c]
        obs = obs.astype(i32)
        terms_of.append(
            [
                (cell & 255).astype(f32),
                (cell >> 8).astype(f32),
                ((obs >> 8) + source * blocks).astype(f32),
                (obs & 255).astype(f32),
                *split(weight),
            ]
        )
    wheres = [position[c : c + 1] for c in range(chunks)]
    sorted_ref[...] = spread_sum(wheres, terms_of, chunks)

    outward.wait()
    passed = [
        started(quarter(2), quarter(2), pass_send.at[by], pass_recv.at[by], mem=ring("mem", by))
        for by in range(1, sharers)
    ]

    groups = [
        (0, own + halo, 0, 2 * blocks),
        (own + halo, chunks, 2 * blocks, (1 + far) * blocks),
    ]
    turns_of, starts, at = [], [], 0
    for low, high, _, _ in groups:
        turns = []
        for b in range(1, buckets):
            below = sum(jnp.where(row < b * TILE, 1, 0) for row in cell_rows[low:high])
            count = jnp.sum(below)
            turns.append(b + lax.shift_right_logical(jnp.maximum(count - 1, 0), 8))
        turns_of.append(turns)
        starts.append(at)
        at += high - low + buckets - 1
    loads[4].wait()
    def weigh(t, near, end, more):
        upper = sorted_ref[pl.ds(2 * chunks + t, 1), :]
        lower = sorted_ref[pl.ds(3 * chunks + t, 1), :]
        total = wide[t] if more else jnp.zeros((levels, TILE), f32)
        for k in range(near, end):
            total += jnp.dot(
                wall_ref[:, k * TILE : (k + 1) * TILE],
                onehot(jnp.where(upper == k, lower, -1.0), TILE),
                preferred_element_type=f32,
            )
        wide[t] = total

    def weigh_all(low, high, near, end, more=False):
        def body(t, carry):
            weigh(t, near, end, more)
            return carry

        lax.fori_loop(low, high, body, 0, unroll=largest_divisor(high - low, 9))

    forward = None
    replies = []
    for number, ((low, high, near, end), turns, start) in enumerate(
        zip(groups, turns_of, starts)
    ):
        if number == 0:
            near_wall.wait()
            weigh_all(low, high, near, end)
        else:
            inward.wait()
            weigh_all(low, high, near, end - blocks)
            forward.wait()
            weigh_all(low, high, end - blocks, end, more=True)

        def pick(i, carry):
            b = bucket_at(turns, i)
            t = low + i - b
            held = sorted_ref[pl.ds(chunks + t, 1), :] == b.astype(f32)
            row = jnp.where(held, sorted_ref[pl.ds(t, 1), :], -1.0)
            columns = jnp.dot(
                state_ref[:, pl.ds(b * TILE, TILE)], onehot(row, TILE), preferred_element_type=f32
            ).reshape(members, levels, TILE)
            dots_ref[start + i, :members] = jnp.sum(columns * wide[t][None], axis=1)
            return carry

        steps = high - low + buckets - 1
        lax.fori_loop(0, steps, pick, 0, unroll=largest_divisor(steps, 8))
        if number == 0:
            for copy in passed:
                copy.wait()
            forward = started(
                whole_wall(2), whole_wall(4), wall_send.at[4], wall_recv.at[4], cell=cell_of[1]
            )

        total = jnp.zeros(((end - near) * 32, TILE), f32)
        for t in range(low, high):
            upper = sorted_ref[2 * chunks + t : 2 * chunks + t + 1, :]
            lower = sorted_ref[3 * chunks + t : 3 * chunks + t + 1, :]
            weight = (
                sorted_ref[4 * chunks + t : 4 * chunks + t + 1, :]
                + sorted_ref[5 * chunks + t : 5 * chunks + t + 1, :]
            )
            dots = jnp.zeros((members, TILE), f32)
            for b in range(buckets):
                at = t - low + b
                here_b = (bucket_at(turns, at) == b).astype(i32).astype(f32)
                dots += here_b * dots_ref[start + at, :members]
            dots = jnp.concatenate(
                [dots * weight, jnp.zeros((16 - members, TILE), f32)], axis=0
            )
            both = jnp.concatenate(split(dots), axis=0).astype(bf16)
            key = row16(upper)[:1]
            left = jnp.concatenate(
                [jnp.where(key == bf16(k), both, bf16(0)) for k in range(near, end)], axis=0
            )
            total += lax.dot_general(left, onehot(lower, TILE), NT, preferred_element_type=f32)
        for k in range(near, end):
            at = (k - near) * 32
            piece = total[at : at + 16] + total[at + 16 : at + 32]
            source, lanes = k // blocks, k % blocks * TILE
            equiv[source, lanes // share, :, lanes % share : lanes % share + TILE] = piece[
                :members
            ]
        for source in range(near // blocks, end // blocks):
            for by in range(sharers):
                if source or by:
                    target = ring("mem", by)
                    replies.append(
                        started(
                            equiv.at[source, target],
                            gathered.at[source, member],
                            equiv_send.at[source * sharers + by],
                            equiv_recv.at[source * sharers + by],
                            mem=target,
                            cell=cell_of[source],
                        )
                    )

    for load in loads[5:]:
        load.wait()
    lanes = pl.ds(pl.multiple_of(member * share, 128), share)
    error = error_ref[:, lanes]
    inverse = 1.0 / (error * error)
    region = region_ref[:, lanes] - (here - 1) * REG_DEV
    region = jnp.where(region < 0, region + patches * REG_DEV, region)
    region = jnp.where(region >= patches * REG_DEV, region - patches * REG_DEV, region)
    gathered[0, member] = equiv[0, member]
    for copy in replies:
        copy.wait()
    whole = []
    for m in range(sharers):
        piece = gathered[0, m]
        for source in range(1, 1 + far):
            piece = piece + gathered[source, m]
        whole.append(piece)
    whole = jnp.concatenate(whole, axis=0)
    everyone = whole.shape[0]
    mean = jnp.sum(whole, axis=0, keepdims=True) * (1.0 / everyone)
    spread = whole - mean
    innov = value_ref[:, lanes] - mean
    right = jnp.concatenate([spread, innov], axis=0) * inverse
    width = sums.shape[-1] // 2
    blank = jnp.zeros((width - everyone - 1, share), f32)
    right = [jnp.concatenate([x, blank], axis=0) for x in split(right)]
    zero = jnp.zeros((width, share), f32)
    ids = lax.broadcasted_iota(i32, (REG_DEV, share), 0)
    hits = [ids + part * REG_DEV == region for part in range(3)]
    product = functools.partial(lax.dot_general, dimension_numbers=NT, preferred_element_type=f32)
    half = members // 2
    result = None
    for side in range(2):
        rights = [
            jnp.concatenate([x, zero] if side == 0 else [zero, x], axis=0).astype(bf16)
            for x in right
        ]
        lefts = []
        for piece in split(spread):
            lefts.append(
                jnp.concatenate(
                    [
                        jnp.where(hit, piece[at : at + 1], 0.0)
                        for m in range(sharers)
                        for hit in hits
                        for at in range(m * members + side * half, m * members + (side + 1) * half)
                    ],
                    axis=0,
                ).astype(bf16)
            )
        part = (
            product(lefts[0], rights[0])
            + product(lefts[0], rights[1])
            + product(lefts[1], rights[0])
        )
        result = part if result is None else result + part
    sums[...] = result.reshape(sums.shape)
    copies = []
    for by in range(sharers):
        target = ring("mem", by)
        for part in range(3):
            if by or part != 1:
                number = by * 3 + part
                copies.append(
                    started(
                        sums.at[target, part],
                        shares.at[member, part],
                        sums_send.at[number],
                        sums_recv.at[number],
                        mem=target,
                        cell=ring("cell", part - 1),
                    )
                )
    shares[member, 1] = sums[member, 1]
    for copy in copies:
        copy.wait()
    final = shares[0, 0]
    for m in range(sharers):
        for part in range(3):
            if m or part:
                final = final + shares[m, part]
    out_ref[...] = final


def unpack_kernel(everyone, final_ref, cov_ref, proj_ref):
    width = final_ref.shape[1] // 2
    half = final_ref.shape[0] // REG_DEV
    members = 2 * half
    final = final_ref[...].reshape(half, REG_DEV, 2 * width)
    cov_ref[:half] = final[:, :, :everyone]
    cov_ref[half:] = final[:, :, width : width + everyone]
    lanes = lax.broadcasted_iota(i32, (REG_DEV, members), 1)
    proj = jnp.zeros((REG_DEV, members), f32)
    for m in range(members):
        at = everyone + m // half * width
        proj = jnp.where(lanes == m, final[m % half, :, at : at + 1], proj)
    proj_ref[...] = proj


def on_device(
    state,
    vertical_weight,
    horizontal_weight,
    obs_slot,
    request_cell,
    obs_value,
    obs_error,
    obs_region,
):
    sharers = lax.axis_size("mem")
    cell_dev, members, levels = state.shape
    obs_dev, neigh = obs_slot.shape
    own = obs_dev // TILE
    halo = 3 * obs_dev // 4 // TILE
    far = len(MOVES)
    chunks = own + far * halo
    sources = 1 + far
    buckets = cell_dev // TILE
    steps = chunks + 2 * (buckets - 1)
    share = obs_dev // sharers
    everyone = sharers * members
    width = everyone + 1 + (-(everyone + 1)) % 16
    rows = members // 2 * REG_DEV
    dma = lambda n: pltpu.SemaphoreType.DMA((n,))
    final = pl.pallas_call(
        functools.partial(kernel, own, halo),
        out_shape=jax.ShapeDtypeStruct((rows, 2 * width), f32),
        in_specs=[HBM] * 8,
        out_specs=VMEM,
        scratch_shapes=[
            pltpu.VMEM((chunks, 1, TILE), i32),
            pltpu.VMEM((neigh, obs_dev), i32),
            pltpu.VMEM((neigh, obs_dev), f32),
            pltpu.VMEM((levels, sources * obs_dev), bf16),
            pltpu.VMEM((members * levels, cell_dev), bf16),
            pltpu.VMEM((1, obs_dev), f32),
            pltpu.VMEM((1, obs_dev), f32),
            pltpu.VMEM((1, obs_dev), i32),
            pltpu.VMEM((chunks, 1, TILE), i32),
            pltpu.VMEM((2, chunks, 1, TILE), f32),
            pltpu.VMEM((2, chunks, 1, TILE), f32),
            pltpu.VMEM((6 * chunks, TILE), f32),
            pltpu.VMEM((chunks, levels, TILE), f32),
            pltpu.VMEM((steps, 16, TILE), f32),
            pltpu.VMEM((sources, sharers, members, share), f32),
            pltpu.VMEM((sources, sharers, members, share), f32),
            pltpu.VMEM((sharers, 3, rows, 2 * width), f32),
            pltpu.VMEM((sharers, 3, rows, 2 * width), f32),
            dma(8),
            dma(5),
            dma(5),
            dma(5),
            dma(5),
            dma(sharers),
            dma(sharers),
            dma(5),
            dma(5),
            dma(sources * sharers),
            dma(sources * sharers),
            dma(3 * sharers),
            dma(3 * sharers),
        ],
        compiler_params=pltpu.CompilerParams(
            collective_id=0, has_side_effects=True, vmem_limit_bytes=60 * 2**20
        ),
    )(
        request_cell.reshape(chunks, 1, TILE),
        obs_slot.T,
        horizontal_weight.T,
        vertical_weight.T,
        state.transpose(1, 2, 0).reshape(members * levels, cell_dev),
        obs_value.reshape(1, obs_dev),
        obs_error.reshape(1, obs_dev),
        obs_region.reshape(1, obs_dev),
    )
    cov, proj = pl.pallas_call(
        functools.partial(unpack_kernel, everyone),
        out_shape=(
            jax.ShapeDtypeStruct((members, REG_DEV, everyone), f32),
            jax.ShapeDtypeStruct((REG_DEV, members), f32),
        ),
        in_specs=[VMEM],
        out_specs=(VMEM, VMEM),
    )(final)
    return cov.transpose(1, 0, 2), proj


def solution(mesh):
    in_specs = (
        P("cell", "mem", None),
        P("cell", None),
        P("cell", None),
        P("cell", None),
        P("cell", None),
        P("cell"),
        P("cell"),
        P("cell"),
    )
    out_specs = (P("cell", "mem", None), P("cell", "mem"))
    return jax.shard_map(
        on_device, mesh=mesh, in_specs=in_specs, out_specs=out_specs, check_vma=False
    )
```

```python
import functools

import jax
import jax.numpy as jnp
from jax import lax
from jax.experimental import pallas as pl
from jax.experimental.pallas import tpu as pltpu
from jax.sharding import PartitionSpec as P

REG_DEV = 8
TILE = 256
MOVES = (-2, -1, 1, 2)
HBM = pl.BlockSpec(memory_space=pltpu.HBM)
MESH = pl.DeviceIdType.MESH
VMEM = pl.BlockSpec(memory_space=pltpu.VMEM)
NT = (((1,), (1,)), ((), ()))
f32, bf16, i32 = jnp.float32, jnp.bfloat16, jnp.int32


def split(x):
    top = x.astype(bf16).astype(f32)
    return top, x - top


def row16(row):
    return jnp.broadcast_to(row, (16, row.shape[1])).astype(bf16)


def onehot(row, count):
    lanes = row.shape[1]
    ids = lax.broadcasted_iota(i32, (count, lanes), 0).astype(f32).astype(bf16)
    hit = ids.reshape(count // 16, 16, lanes) == row16(row)[None]
    return jnp.where(hit, bf16(1), bf16(0)).reshape(count, lanes)


def spread_rows(row, value, count):
    ids = lax.broadcasted_iota(i32, (count, row.shape[1]), 0).astype(f32)
    return jnp.where(ids == row, value, 0.0)


def ring(axis, by):
    return lax.rem(lax.axis_index(axis) + by + lax.axis_size(axis), lax.axis_size(axis))


def remote(src, dst, send, recv, **target):
    return pltpu.make_async_remote_copy(
        src_ref=src,
        dst_ref=dst,
        send_sem=send,
        recv_sem=recv,
        device_id=target,
        device_id_type=MESH,
    )


def started(*args, **target):
    copy = remote(*args, **target)
    copy.start()
    return copy


def spread_sum(wheres, terms_of, count):
    total = None
    for where, terms in zip(wheres, terms_of):
        high = (where >> 8).astype(f32)
        left = jnp.concatenate([spread_rows(high, t, count) for t in terms], axis=0)
        part = lax.dot_general(
            left.astype(bf16),
            onehot((where & 255).astype(f32), TILE),
            NT,
            preferred_element_type=f32,
        )
        total = part if total is None else total + part
    return total


def bucket_at(turns, i):
    b = i32(0)
    for turn in turns:
        b += jnp.where(i >= turn, 1, 0)
    return b


def largest_divisor(n, most):
    return max(u for u in range(1, most + 1) if n % u == 0)


def kernel(
    own,
    halo,
    table_hbm,
    slot_hbm,
    h_hbm,
    w_hbm,
    state_hbm,
    value_hbm,
    error_hbm,
    region_hbm,
    out_ref,
    table_ref,
    slot_ref,
    h_ref,
    wall_ref,
    state_ref,
    value_ref,
    error_ref,
    region_ref,
    cells,
    sent,
    got,
    sorted_ref,
    wide,
    dots_ref,
    equiv,
    gathered,
    sums,
    shares,
    load_sem,
    cell_send,
    cell_recv,
    wall_send,
    wall_recv,
    pass_send,
    pass_recv,
    note_send,
    note_recv,
    equiv_send,
    equiv_recv,
    sums_send,
    sums_recv,
):
    far = len(MOVES)
    chunks = own + far * halo
    levels, obs_dev = w_hbm.shape
    members = state_hbm.shape[0] // levels
    blocks = obs_dev // TILE
    buckets = state_hbm.shape[1] // TILE
    patches, sharers = lax.axis_size("cell"), lax.axis_size("mem")
    here, member = lax.axis_index("cell"), lax.axis_index("mem")
    share = obs_dev // sharers

    loads = []
    for number, (src, dst) in enumerate(
        (
            (table_hbm, table_ref),
            (w_hbm, wall_ref.at[:, :obs_dev]),
            (slot_hbm, slot_ref),
            (h_hbm, h_ref),
            (state_hbm, state_ref),
            (value_hbm, value_ref),
            (error_hbm, error_ref),
            (region_hbm, region_ref),
        )
    ):
        copy = pltpu.make_async_copy(src, dst, load_sem.at[number])
        copy.start()
        loads.append(copy)
    barrier = pltpu.get_barrier_semaphore()
    greeted = [(0, c) for c in MOVES] + [(m, 0) for m in range(1, sharers)]
    for m, c in greeted:
        pl.semaphore_signal(
            barrier,
            inc=1,
            device_id={"mem": ring("mem", m), "cell": ring("cell", c)},
            device_id_type=MESH,
        )

    even = 1 - lax.rem(here, 2)
    outer = 1 - 2 * even
    offsets = (0, -outer, outer, 2 * outer, -2 * outer)
    asked = (0, -outer, outer, -2 * outer, 2 * outer)
    part_of = (0, 1 + even, 2 - even, 3 * even, 3 - 3 * even)
    cell_of = [ring("cell", by) for by in offsets]
    asked_of = [ring("cell", by) for by in asked]

    loads[2].wait()
    loads[3].wait()
    lane = lax.broadcasted_iota(i32, (1, TILE), 1).astype(f32)
    wheres, terms_of = [], []
    for k in range(slot_ref.shape[0]):
        for j in range(blocks):
            tops, rest = split(h_ref[k : k + 1, j * TILE : (j + 1) * TILE])
            wheres.append(slot_ref[k : k + 1, j * TILE : (j + 1) * TILE])
            terms_of.append([jnp.full((1, TILE), float(j), f32), lane, tops, rest])
    by_slot = spread_sum(wheres, terms_of, chunks)
    slot_obs = by_slot[:chunks] * TILE + by_slot[chunks : 2 * chunks]
    slot_h = by_slot[2 * chunks : 3 * chunks] + by_slot[3 * chunks :]
    for c in range(chunks):
        sent[0, c] = slot_obs[c : c + 1]
        sent[1, c] = slot_h[c : c + 1]
    loads[0].wait()
    loads[1].wait()
    pl.semaphore_wait(barrier, len(greeted))

    def segment(k):
        return pl.ds(own + part_of[k] * halo, halo)

    def landing(k):
        return pl.ds(own + (k - 1) * halo, halo)

    first = [
        started(
            table_ref.at[segment(k)],
            cells.at[landing(k)],
            cell_send.at[k],
            cell_recv.at[k],
            cell=asked_of[k],
        )
        for k in range(1, 1 + far)
    ]
    second = [
        started(
            sent.at[:, segment(k)],
            got.at[:, landing(k)],
            note_send.at[k],
            note_recv.at[k],
            cell=asked_of[k],
        )
        for k in range(1, 1 + far)
    ]

    def quarter(k):
        return wall_ref.at[:, pl.ds(pl.multiple_of(k * obs_dev + member * share, 128), share)]

    def whole_wall(k):
        return wall_ref.at[:, k * obs_dev : (k + 1) * obs_dev]

    outward = started(
        quarter(0), quarter(2), wall_send.at[2], wall_recv.at[2], cell=asked_of[2]
    )
    near_wall = started(
        whole_wall(0), whole_wall(1), wall_send.at[1], wall_recv.at[1], cell=asked_of[1]
    )
    inward = started(
        whole_wall(0), whole_wall(3), wall_send.at[3], wall_recv.at[3], cell=asked_of[3]
    )

    for copy in first:
        copy.wait()
    cell_rows = [table_ref[c] if c < own else cells[c] for c in range(chunks)]
    bucket_ids = lax.broadcasted_iota(i32, (8, TILE), 0)
    member_of = jnp.concatenate(
        [jnp.where(bucket_ids == (row >> 8), 1.0, 0.0) for row in cell_rows], axis=0
    )
    rows = 8 * chunks
    place = lax.broadcasted_iota(i32, (TILE, TILE), 0) < lax.broadcasted_iota(i32, (TILE, TILE), 1)
    within = jnp.dot(
        member_of.astype(bf16), jnp.where(place, 1.0, 0.0).astype(bf16), preferred_element_type=f32
    )

    def order(axis):
        index = lax.broadcasted_iota(i32, (rows, rows), axis)
        chunk = index >> 3
        late = jnp.where(chunk >= own + halo, 1, 0)
        return (late * 8 + (index & 7)) * chunks + chunk

    before = jnp.where(order(1) < order(0), 1.0, 0.0).astype(bf16)
    ahead = jnp.dot(before, member_of.astype(bf16), preferred_element_type=f32)
    base = jnp.sum(ahead, axis=1, keepdims=True)
    position = jnp.sum(((within + base) * member_of).reshape(chunks, 8, TILE), axis=1)
    position = position.astype(i32)
    for copy in second:
        copy.wait()
    terms_of = []
    for c, cell in enumerate(cell_rows):
        if c < own:
            source, obs, weight = 0, slot_obs[c : c + 1], slot_h[c : c + 1]
        else:
            source, obs, weight = 1 + (c - own) // halo, got[0, c], got[1, c]
        obs = obs.astype(i32)
        terms_of.append(
            [
                (cell & 255).astype(f32),
                (cell >> 8).astype(f32),
                ((obs >> 8) + source * blocks).astype(f32),
                (obs & 255).astype(f32),
                *split(weight),
            ]
        )
    wheres = [position[c : c + 1] for c in range(chunks)]
    sorted_ref[...] = spread_sum(wheres, terms_of, chunks)

    outward.wait()
    passed = [
        started(quarter(2), quarter(2), pass_send.at[by], pass_recv.at[by], mem=ring("mem", by))
        for by in range(1, sharers)
    ]

    groups = [
        (0, own + halo, 0, 2 * blocks),
        (own + halo, chunks, 2 * blocks, (1 + far) * blocks),
    ]
    turns_of, starts, at = [], [], 0
    for low, high, _, _ in groups:
        turns = []
        for b in range(1, buckets):
            below = sum(jnp.where(row < b * TILE, 1, 0) for row in cell_rows[low:high])
            count = jnp.sum(below)
            turns.append(b + lax.shift_right_logical(jnp.maximum(count - 1, 0), 8))
        turns_of.append(turns)
        starts.append(at)
        at += high - low + buckets - 1
    loads[4].wait()
    def weigh(t, near, end, more):
        upper = sorted_ref[pl.ds(2 * chunks + t, 1), :]
        lower = sorted_ref[pl.ds(3 * chunks + t, 1), :]
        total = wide[t] if more else jnp.zeros((levels, TILE), f32)
        for k in range(near, end):
            total += jnp.dot(
                wall_ref[:, k * TILE : (k + 1) * TILE],
                onehot(jnp.where(upper == k, lower, -1.0), TILE),
                preferred_element_type=f32,
            )
        wide[t] = total

    def weigh_all(low, high, near, end, more=False):
        def body(t, carry):
            weigh(t, near, end, more)
            return carry

        lax.fori_loop(low, high, body, 0, unroll=largest_divisor(high - low, 9))

    forward = None
    replies = []
    for number, ((low, high, near, end), turns, start) in enumerate(
        zip(groups, turns_of, starts)
    ):
        if number == 0:
            near_wall.wait()
            weigh_all(low, high, near, end)
        else:
            inward.wait()
            weigh_all(low, high, near, end - blocks)
            forward.wait()
            weigh_all(low, high, end - blocks, end, more=True)

        def pick(i, carry):
            b = bucket_at(turns, i)
            t = low + i - b
            held = sorted_ref[pl.ds(chunks + t, 1), :] == b.astype(f32)
            row = jnp.where(held, sorted_ref[pl.ds(t, 1), :], -1.0)
            columns = jnp.dot(
                state_ref[:, pl.ds(b * TILE, TILE)], onehot(row, TILE), preferred_element_type=f32
            ).reshape(members, levels, TILE)
            dots_ref[start + i, :members] = jnp.sum(columns * wide[t][None], axis=1)
            return carry

        steps = high - low + buckets - 1
        lax.fori_loop(0, steps, pick, 0, unroll=largest_divisor(steps, 8))
        if number == 0:
            for copy in passed:
                copy.wait()
            forward = started(
                whole_wall(2), whole_wall(4), wall_send.at[4], wall_recv.at[4], cell=cell_of[1]
            )

    for number in (1, 0):
        (low, high, near, end), turns, start = groups[number], turns_of[number], starts[number]
        total = jnp.zeros(((end - near) * 32, TILE), f32)
        for t in range(low, high):
            upper = sorted_ref[2 * chunks + t : 2 * chunks + t + 1, :]
            lower = sorted_ref[3 * chunks + t : 3 * chunks + t + 1, :]
            weight = (
                sorted_ref[4 * chunks + t : 4 * chunks + t + 1, :]
                + sorted_ref[5 * chunks + t : 5 * chunks + t + 1, :]
            )
            dots = jnp.zeros((members, TILE), f32)
            for b in range(buckets):
                at = t - low + b
                here_b = (bucket_at(turns, at) == b).astype(i32).astype(f32)
                dots += here_b * dots_ref[start + at, :members]
            dots = jnp.concatenate(
                [dots * weight, jnp.zeros((16 - members, TILE), f32)], axis=0
            )
            both = jnp.concatenate(split(dots), axis=0).astype(bf16)
            key = row16(upper)[:1]
            left = jnp.concatenate(
                [jnp.where(key == bf16(k), both, bf16(0)) for k in range(near, end)], axis=0
            )
            total += lax.dot_general(left, onehot(lower, TILE), NT, preferred_element_type=f32)
        for k in range(near, end):
            at = (k - near) * 32
            piece = total[at : at + 16] + total[at + 16 : at + 32]
            source, block = k // blocks, k % blocks * (TILE // 128)
            for part in range(TILE // 128):
                row = (block + part) % (share // 128) * members
                equiv[source, (block + part) // (share // 128), row : row + members] = piece[
                    :members, part * 128 : (part + 1) * 128
                ]
        for source in range(near // blocks, end // blocks):
            for by in range(sharers):
                if source or by:
                    target = ring("mem", by)
                    replies.append(
                        started(
                            equiv.at[source, target],
                            gathered.at[source, member],
                            equiv_send.at[source * sharers + by],
                            equiv_recv.at[source * sharers + by],
                            mem=target,
                            cell=cell_of[source],
                        )
                    )

    for load in loads[5:]:
        load.wait()
    lanes = pl.ds(pl.multiple_of(member * share, 128), share)
    error = error_ref[:, lanes]
    inverse = 1.0 / (error * error)
    region = region_ref[:, lanes] - (here - 1) * REG_DEV
    region = jnp.where(region < 0, region + patches * REG_DEV, region)
    region = jnp.where(region >= patches * REG_DEV, region - patches * REG_DEV, region)
    gathered[0, member] = equiv[0, member]
    for copy in replies:
        copy.wait()
    whole = []
    for m in range(sharers):
        piece = gathered[0, m]
        for source in range(1, 1 + far):
            piece = piece + gathered[source, m]
        piece = [piece[at : at + members] for at in range(0, piece.shape[0], members)]
        whole.append(jnp.concatenate(piece, axis=1))
    whole = jnp.concatenate(whole, axis=0)
    everyone = whole.shape[0]
    mean = jnp.sum(whole, axis=0, keepdims=True) * (1.0 / everyone)
    spread = whole - mean
    innov = value_ref[:, lanes] - mean
    right = jnp.concatenate([spread, innov], axis=0) * inverse
    width = sums.shape[-1] // 2
    blank = jnp.zeros((width - everyone - 1, share), f32)
    right = [jnp.concatenate([x, blank], axis=0) for x in split(right)]
    zero = jnp.zeros((width, share), f32)
    ids = lax.broadcasted_iota(i32, (REG_DEV, share), 0)
    hits = [ids + part * REG_DEV == region for part in range(3)]
    product = functools.partial(lax.dot_general, dimension_numbers=NT, preferred_element_type=f32)
    half = members // 2
    result = None
    for side in range(2):
        rights = [
            jnp.concatenate([x, zero] if side == 0 else [zero, x], axis=0).astype(bf16)
            for x in right
        ]
        lefts = []
        for piece in split(spread):
            lefts.append(
                jnp.concatenate(
                    [
                        jnp.where(hit, piece[at : at + 1], 0.0)
                        for m in range(sharers)
                        for hit in hits
                        for at in range(m * members + side * half, m * members + (side + 1) * half)
                    ],
                    axis=0,
                ).astype(bf16)
            )
        part = (
            product(lefts[0], rights[0])
            + product(lefts[0], rights[1])
            + product(lefts[1], rights[0])
        )
        result = part if result is None else result + part
    sums[...] = result.reshape(sums.shape)
    copies = []
    for by in range(sharers):
        target = ring("mem", by)
        for part in range(3):
            if by or part != 1:
                number = by * 3 + part
                copies.append(
                    started(
                        sums.at[target, part],
                        shares.at[member, part],
                        sums_send.at[number],
                        sums_recv.at[number],
                        mem=target,
                        cell=ring("cell", part - 1),
                    )
                )
    shares[member, 1] = sums[member, 1]
    for copy in copies:
        copy.wait()
    final = shares[0, 0]
    for m in range(sharers):
        for part in range(3):
            if m or part:
                final = final + shares[m, part]
    out_ref[...] = final


def unpack_kernel(everyone, final_ref, cov_ref, proj_ref):
    width = final_ref.shape[1] // 2
    half = final_ref.shape[0] // REG_DEV
    members = 2 * half
    final = final_ref[...].reshape(half, REG_DEV, 2 * width)
    cov_ref[:half] = final[:, :, :everyone]
    cov_ref[half:] = final[:, :, width : width + everyone]
    lanes = lax.broadcasted_iota(i32, (REG_DEV, members), 1)
    proj = jnp.zeros((REG_DEV, members), f32)
    for m in range(members):
        at = everyone + m // half * width
        proj = jnp.where(lanes == m, final[m % half, :, at : at + 1], proj)
    proj_ref[...] = proj


def on_device(
    state,
    vertical_weight,
    horizontal_weight,
    obs_slot,
    request_cell,
    obs_value,
    obs_error,
    obs_region,
):
    sharers = lax.axis_size("mem")
    cell_dev, members, levels = state.shape
    obs_dev, neigh = obs_slot.shape
    own = obs_dev // TILE
    halo = 3 * obs_dev // 4 // TILE
    far = len(MOVES)
    chunks = own + far * halo
    sources = 1 + far
    buckets = cell_dev // TILE
    steps = chunks + 2 * (buckets - 1)
    share = obs_dev // sharers
    everyone = sharers * members
    width = everyone + 1 + (-(everyone + 1)) % 16
    rows = members // 2 * REG_DEV
    dma = lambda n: pltpu.SemaphoreType.DMA((n,))
    final = pl.pallas_call(
        functools.partial(kernel, own, halo),
        out_shape=jax.ShapeDtypeStruct((rows, 2 * width), f32),
        in_specs=[HBM] * 8,
        out_specs=VMEM,
        scratch_shapes=[
            pltpu.VMEM((chunks, 1, TILE), i32),
            pltpu.VMEM((neigh, obs_dev), i32),
            pltpu.VMEM((neigh, obs_dev), f32),
            pltpu.VMEM((levels, sources * obs_dev), bf16),
            pltpu.VMEM((members * levels, cell_dev), bf16),
            pltpu.VMEM((1, obs_dev), f32),
            pltpu.VMEM((1, obs_dev), f32),
            pltpu.VMEM((1, obs_dev), i32),
            pltpu.VMEM((chunks, 1, TILE), i32),
            pltpu.VMEM((2, chunks, 1, TILE), f32),
            pltpu.VMEM((2, chunks, 1, TILE), f32),
            pltpu.VMEM((6 * chunks, TILE), f32),
            pltpu.VMEM((chunks, levels, TILE), f32),
            pltpu.VMEM((steps, 16, TILE), f32),
            pltpu.VMEM((sources, sharers, members * share // 128, 128), f32),
            pltpu.VMEM((sources, sharers, members * share // 128, 128), f32),
            pltpu.VMEM((sharers, 3, rows, 2 * width), f32),
            pltpu.VMEM((sharers, 3, rows, 2 * width), f32),
            dma(8),
            dma(5),
            dma(5),
            dma(5),
            dma(5),
            dma(sharers),
            dma(sharers),
            dma(5),
            dma(5),
            dma(sources * sharers),
            dma(sources * sharers),
            dma(3 * sharers),
            dma(3 * sharers),
        ],
        compiler_params=pltpu.CompilerParams(
            collective_id=0, has_side_effects=True, vmem_limit_bytes=60 * 2**20
        ),
    )(
        request_cell.reshape(chunks, 1, TILE),
        obs_slot.T,
        horizontal_weight.T,
        vertical_weight.T,
        state.transpose(1, 2, 0).reshape(members * levels, cell_dev),
        obs_value.reshape(1, obs_dev),
        obs_error.reshape(1, obs_dev),
        obs_region.reshape(1, obs_dev),
    )
    cov, proj = pl.pallas_call(
        functools.partial(unpack_kernel, everyone),
        out_shape=(
            jax.ShapeDtypeStruct((members, REG_DEV, everyone), f32),
            jax.ShapeDtypeStruct((REG_DEV, members), f32),
        ),
        in_specs=[VMEM],
        out_specs=(VMEM, VMEM),
    )(final)
    return cov.transpose(1, 0, 2), proj


def solution(mesh):
    in_specs = (
        P("cell", "mem", None),
        P("cell", None),
        P("cell", None),
        P("cell", None),
        P("cell", None),
        P("cell"),
        P("cell"),
        P("cell"),
    )
    out_specs = (P("cell", "mem", None), P("cell", "mem"))
    return jax.shard_map(
        on_device, mesh=mesh, in_specs=in_specs, out_specs=out_specs, check_vma=False
    )
```

```python
import functools

import jax
import jax.numpy as jnp
from jax import lax
from jax.experimental import pallas as pl
from jax.experimental.pallas import tpu as pltpu
from jax.sharding import PartitionSpec as P

REG_DEV = 8
TILE = 256
MOVES = (-2, -1, 1, 2)
HBM = pl.BlockSpec(memory_space=pltpu.HBM)
MESH = pl.DeviceIdType.MESH
VMEM = pl.BlockSpec(memory_space=pltpu.VMEM)
NT = (((1,), (1,)), ((), ()))
f32, bf16, i32 = jnp.float32, jnp.bfloat16, jnp.int32


def split(x):
    top = x.astype(bf16).astype(f32)
    return top, x - top


def row16(row):
    return jnp.broadcast_to(row, (16, row.shape[1])).astype(bf16)


def onehot(row, count):
    lanes = row.shape[1]
    ids = lax.broadcasted_iota(i32, (count, lanes), 0).astype(f32).astype(bf16)
    hit = ids.reshape(count // 16, 16, lanes) == row16(row)[None]
    return jnp.where(hit, bf16(1), bf16(0)).reshape(count, lanes)


def spread_rows(row, value, count):
    ids = lax.broadcasted_iota(i32, (count, row.shape[1]), 0).astype(f32)
    return jnp.where(ids == row, value, 0.0)


def ring(axis, by):
    return lax.rem(lax.axis_index(axis) + by + lax.axis_size(axis), lax.axis_size(axis))


def remote(src, dst, send, recv, **target):
    return pltpu.make_async_remote_copy(
        src_ref=src,
        dst_ref=dst,
        send_sem=send,
        recv_sem=recv,
        device_id=target,
        device_id_type=MESH,
    )


def started(*args, **target):
    copy = remote(*args, **target)
    copy.start()
    return copy


def spread_sum(wheres, terms_of, count):
    total = None
    for where, terms in zip(wheres, terms_of):
        high = (where >> 8).astype(f32)
        left = jnp.concatenate([spread_rows(high, t, count) for t in terms], axis=0)
        part = lax.dot_general(
            left.astype(bf16),
            onehot((where & 255).astype(f32), TILE),
            NT,
            preferred_element_type=f32,
        )
        total = part if total is None else total + part
    return total


def bucket_at(turns, i):
    b = i32(0)
    for turn in turns:
        b += jnp.where(i >= turn, 1, 0)
    return b


def largest_divisor(n, most):
    return max(u for u in range(1, most + 1) if n % u == 0)


def kernel(
    own,
    halo,
    table_hbm,
    slot_hbm,
    h_hbm,
    w_hbm,
    state_hbm,
    value_hbm,
    error_hbm,
    region_hbm,
    out_ref,
    table_ref,
    slot_ref,
    h_ref,
    wall_ref,
    state_ref,
    value_ref,
    error_ref,
    region_ref,
    cells,
    sent,
    got,
    sorted_ref,
    wide,
    dots_ref,
    equiv,
    gathered,
    sums,
    shares,
    load_sem,
    cell_send,
    cell_recv,
    wall_send,
    wall_recv,
    pass_send,
    pass_recv,
    note_send,
    note_recv,
    equiv_send,
    equiv_recv,
    sums_send,
    sums_recv,
):
    far = len(MOVES)
    chunks = own + far * halo
    levels, obs_dev = w_hbm.shape
    members = state_hbm.shape[0] // levels
    blocks = obs_dev // TILE
    buckets = state_hbm.shape[1] // TILE
    patches, sharers = lax.axis_size("cell"), lax.axis_size("mem")
    here, member = lax.axis_index("cell"), lax.axis_index("mem")
    share = obs_dev // sharers

    loads = []
    for number, (src, dst) in enumerate(
        (
            (table_hbm, table_ref),
            (w_hbm, wall_ref.at[:, :obs_dev]),
            (slot_hbm, slot_ref),
            (h_hbm, h_ref),
            (state_hbm, state_ref),
            (value_hbm, value_ref),
            (error_hbm, error_ref),
            (region_hbm, region_ref),
        )
    ):
        copy = pltpu.make_async_copy(src, dst, load_sem.at[number])
        copy.start()
        loads.append(copy)
    barrier = pltpu.get_barrier_semaphore()
    greeted = [(0, c) for c in MOVES] + [(m, 0) for m in range(1, sharers)]
    for m, c in greeted:
        pl.semaphore_signal(
            barrier,
            inc=1,
            device_id={"mem": ring("mem", m), "cell": ring("cell", c)},
            device_id_type=MESH,
        )

    even = 1 - lax.rem(here, 2)
    outer = 1 - 2 * even
    offsets = (0, -outer, 2 * outer, outer, -2 * outer)
    asked = (0, -outer, -2 * outer, outer, 2 * outer)
    part_of = (0, 1 + even, 3 * even, 2 - even, 3 - 3 * even)
    cell_of = [ring("cell", by) for by in offsets]
    asked_of = [ring("cell", by) for by in asked]

    loads[2].wait()
    loads[3].wait()
    lane = lax.broadcasted_iota(i32, (1, TILE), 1).astype(f32)
    wheres, terms_of = [], []
    for k in range(slot_ref.shape[0]):
        for j in range(blocks):
            tops, rest = split(h_ref[k : k + 1, j * TILE : (j + 1) * TILE])
            wheres.append(slot_ref[k : k + 1, j * TILE : (j + 1) * TILE])
            terms_of.append([jnp.full((1, TILE), float(j), f32), lane, tops, rest])
    by_slot = spread_sum(wheres, terms_of, chunks)
    slot_obs = by_slot[:chunks] * TILE + by_slot[chunks : 2 * chunks]
    slot_h = by_slot[2 * chunks : 3 * chunks] + by_slot[3 * chunks :]
    for c in range(chunks):
        sent[0, c] = slot_obs[c : c + 1]
        sent[1, c] = slot_h[c : c + 1]
    loads[0].wait()
    loads[1].wait()
    pl.semaphore_wait(barrier, len(greeted))

    def segment(k):
        return pl.ds(own + part_of[k] * halo, halo)

    def landing(k):
        return pl.ds(own + (k - 1) * halo, halo)

    first = [
        started(
            table_ref.at[segment(k)],
            cells.at[landing(k)],
            cell_send.at[k],
            cell_recv.at[k],
            cell=asked_of[k],
        )
        for k in range(1, 1 + far)
    ]
    second = [
        started(
            sent.at[:, segment(k)],
            got.at[:, landing(k)],
            note_send.at[k],
            note_recv.at[k],
            cell=asked_of[k],
        )
        for k in range(1, 1 + far)
    ]

    def quarter(k):
        return wall_ref.at[:, pl.ds(pl.multiple_of(k * obs_dev + member * share, 128), share)]

    def whole_wall(k):
        return wall_ref.at[:, k * obs_dev : (k + 1) * obs_dev]

    outward = started(
        quarter(0), quarter(3), wall_send.at[3], wall_recv.at[3], cell=asked_of[3]
    )
    near_wall = started(
        whole_wall(0), whole_wall(1), wall_send.at[1], wall_recv.at[1], cell=asked_of[1]
    )
    inward = started(
        whole_wall(0), whole_wall(2), wall_send.at[2], wall_recv.at[2], cell=asked_of[2]
    )

    for copy in first:
        copy.wait()
    cell_rows = [table_ref[c] if c < own else cells[c] for c in range(chunks)]
    bucket_ids = lax.broadcasted_iota(i32, (8, TILE), 0)
    member_of = jnp.concatenate(
        [jnp.where(bucket_ids == (row >> 8), 1.0, 0.0) for row in cell_rows], axis=0
    )
    rows = 8 * chunks
    place = lax.broadcasted_iota(i32, (TILE, TILE), 0) < lax.broadcasted_iota(i32, (TILE, TILE), 1)
    within = jnp.dot(
        member_of.astype(bf16), jnp.where(place, 1.0, 0.0).astype(bf16), preferred_element_type=f32
    )

    def order(axis):
        index = lax.broadcasted_iota(i32, (rows, rows), axis)
        chunk = index >> 3
        late = jnp.where(chunk >= own + halo, 1, 0) + jnp.where(chunk >= own + 2 * halo, 1, 0)
        return (late * 8 + (index & 7)) * chunks + chunk

    before = jnp.where(order(1) < order(0), 1.0, 0.0).astype(bf16)
    ahead = jnp.dot(before, member_of.astype(bf16), preferred_element_type=f32)
    base = jnp.sum(ahead, axis=1, keepdims=True)
    position = jnp.sum(((within + base) * member_of).reshape(chunks, 8, TILE), axis=1)
    position = position.astype(i32)
    for copy in second:
        copy.wait()
    terms_of = []
    for c, cell in enumerate(cell_rows):
        if c < own:
            source, obs, weight = 0, slot_obs[c : c + 1], slot_h[c : c + 1]
        else:
            source, obs, weight = 1 + (c - own) // halo, got[0, c], got[1, c]
        obs = obs.astype(i32)
        terms_of.append(
            [
                (cell & 255).astype(f32),
                (cell >> 8).astype(f32),
                ((obs >> 8) + source * blocks).astype(f32),
                (obs & 255).astype(f32),
                *split(weight),
            ]
        )
    wheres = [position[c : c + 1] for c in range(chunks)]
    sorted_ref[...] = spread_sum(wheres, terms_of, chunks)

    outward.wait()
    passed = [
        started(quarter(3), quarter(3), pass_send.at[by], pass_recv.at[by], mem=ring("mem", by))
        for by in range(1, sharers)
    ]

    groups = [
        (0, own + halo, 0, 2 * blocks),
        (own + halo, own + 2 * halo, 2 * blocks, 3 * blocks),
        (own + 2 * halo, chunks, 3 * blocks, (1 + far) * blocks),
    ]
    turns_of, starts, at = [], [], 0
    for low, high, _, _ in groups:
        turns = []
        for b in range(1, buckets):
            below = sum(jnp.where(row < b * TILE, 1, 0) for row in cell_rows[low:high])
            count = jnp.sum(below)
            turns.append(b + lax.shift_right_logical(jnp.maximum(count - 1, 0), 8))
        turns_of.append(turns)
        starts.append(at)
        at += high - low + buckets - 1
    loads[4].wait()
    def weigh(t, near, end, more):
        upper = sorted_ref[pl.ds(2 * chunks + t, 1), :]
        lower = sorted_ref[pl.ds(3 * chunks + t, 1), :]
        total = wide[t] if more else jnp.zeros((levels, TILE), f32)
        for k in range(near, end):
            total += jnp.dot(
                wall_ref[:, k * TILE : (k + 1) * TILE],
                onehot(jnp.where(upper == k, lower, -1.0), TILE),
                preferred_element_type=f32,
            )
        wide[t] = total

    def weigh_all(low, high, near, end, more=False):
        def body(t, carry):
            weigh(t, near, end, more)
            return carry

        lax.fori_loop(low, high, body, 0, unroll=largest_divisor(high - low, 9))

    replies = []

    def answer(number):
        (low, high, near, end), turns, start = groups[number], turns_of[number], starts[number]
        total = jnp.zeros(((end - near) * 32, TILE), f32)
        for t in range(low, high):
            upper = sorted_ref[2 * chunks + t : 2 * chunks + t + 1, :]
            lower = sorted_ref[3 * chunks + t : 3 * chunks + t + 1, :]
            weight = (
                sorted_ref[4 * chunks + t : 4 * chunks + t + 1, :]
                + sorted_ref[5 * chunks + t : 5 * chunks + t + 1, :]
            )
            dots = jnp.zeros((members, TILE), f32)
            for b in range(buckets):
                at = t - low + b
                here_b = (bucket_at(turns, at) == b).astype(i32).astype(f32)
                dots += here_b * dots_ref[start + at, :members]
            dots = jnp.concatenate(
                [dots * weight, jnp.zeros((16 - members, TILE), f32)], axis=0
            )
            both = jnp.concatenate(split(dots), axis=0).astype(bf16)
            key = row16(upper)[:1]
            left = jnp.concatenate(
                [jnp.where(key == bf16(k), both, bf16(0)) for k in range(near, end)], axis=0
            )
            total += lax.dot_general(left, onehot(lower, TILE), NT, preferred_element_type=f32)
        for k in range(near, end):
            at = (k - near) * 32
            piece = total[at : at + 16] + total[at + 16 : at + 32]
            source, block = k // blocks, k % blocks * (TILE // 128)
            for part in range(TILE // 128):
                row = (block + part) % (share // 128) * members
                equiv[source, (block + part) // (share // 128), row : row + members] = piece[
                    :members, part * 128 : (part + 1) * 128
                ]
        for source in range(near // blocks, end // blocks):
            for by in range(sharers):
                if source or by:
                    target = ring("mem", by)
                    replies.append(
                        started(
                            equiv.at[source, target],
                            gathered.at[source, member],
                            equiv_send.at[source * sharers + by],
                            equiv_recv.at[source * sharers + by],
                            mem=target,
                            cell=cell_of[source],
                        )
                    )

    forward = None
    for number, ((low, high, near, end), turns, start) in enumerate(
        zip(groups, turns_of, starts)
    ):
        if number == 0:
            near_wall.wait()
            weigh_all(low, high, near, end)
        elif number == 1:
            inward.wait()
            weigh_all(low, high, near, end)
        else:
            weigh_all(low, high, near, end - blocks)
            forward.wait()
            weigh_all(low, high, end - blocks, end, more=True)

        def pick(i, carry):
            b = bucket_at(turns, i)
            t = low + i - b
            held = sorted_ref[pl.ds(chunks + t, 1), :] == b.astype(f32)
            row = jnp.where(held, sorted_ref[pl.ds(t, 1), :], -1.0)
            columns = jnp.dot(
                state_ref[:, pl.ds(b * TILE, TILE)], onehot(row, TILE), preferred_element_type=f32
            ).reshape(members, levels, TILE)
            dots_ref[start + i, :members] = jnp.sum(columns * wide[t][None], axis=1)
            return carry

        steps = high - low + buckets - 1
        unroll = min(range(5, 9), key=lambda u: (steps % u, -u))
        main = steps - steps % unroll
        lax.fori_loop(0, main, pick, 0, unroll=unroll)
        if main < steps:
            lax.fori_loop(main, steps, pick, 0, unroll=steps - main)
        if number == 1:
            answer(1)
        if number == 0:
            for copy in passed:
                copy.wait()
            forward = started(
                whole_wall(3), whole_wall(4), wall_send.at[4], wall_recv.at[4], cell=cell_of[1]
            )

    answer(2)
    answer(0)

    for load in loads[5:]:
        load.wait()
    lanes = pl.ds(pl.multiple_of(member * share, 128), share)
    error = error_ref[:, lanes]
    inverse = 1.0 / (error * error)
    region = region_ref[:, lanes] - (here - 1) * REG_DEV
    region = jnp.where(region < 0, region + patches * REG_DEV, region)
    region = jnp.where(region >= patches * REG_DEV, region - patches * REG_DEV, region)
    gathered[0, member] = equiv[0, member]
    for copy in replies:
        copy.wait()
    whole = []
    for m in range(sharers):
        piece = gathered[0, m]
        for source in range(1, 1 + far):
            piece = piece + gathered[source, m]
        piece = [piece[at : at + members] for at in range(0, piece.shape[0], members)]
        whole.append(jnp.concatenate(piece, axis=1))
    whole = jnp.concatenate(whole, axis=0)
    everyone = whole.shape[0]
    mean = jnp.sum(whole, axis=0, keepdims=True) * (1.0 / everyone)
    spread = whole - mean
    innov = value_ref[:, lanes] - mean
    right = jnp.concatenate([spread, innov], axis=0) * inverse
    width = sums.shape[-1] // 2
    blank = jnp.zeros((width - everyone - 1, share), f32)
    right = [jnp.concatenate([x, blank], axis=0) for x in split(right)]
    zero = jnp.zeros((width, share), f32)
    ids = lax.broadcasted_iota(i32, (REG_DEV, share), 0)
    hits = [ids + part * REG_DEV == region for part in range(3)]
    product = functools.partial(lax.dot_general, dimension_numbers=NT, preferred_element_type=f32)
    half = members // 2
    result = None
    for side in range(2):
        rights = [
            jnp.concatenate([x, zero] if side == 0 else [zero, x], axis=0).astype(bf16)
            for x in right
        ]
        lefts = []
        for piece in split(spread):
            lefts.append(
                jnp.concatenate(
                    [
                        jnp.where(hit, piece[at : at + 1], 0.0)
                        for m in range(sharers)
                        for hit in hits
                        for at in range(m * members + side * half, m * members + (side + 1) * half)
                    ],
                    axis=0,
                ).astype(bf16)
            )
        part = (
            product(lefts[0], rights[0])
            + product(lefts[0], rights[1])
            + product(lefts[1], rights[0])
        )
        result = part if result is None else result + part
    sums[...] = result.reshape(sums.shape)
    copies = []
    for by in range(sharers):
        target = ring("mem", by)
        for part in range(3):
            if by or part != 1:
                number = by * 3 + part
                copies.append(
                    started(
                        sums.at[target, part],
                        shares.at[member, part],
                        sums_send.at[number],
                        sums_recv.at[number],
                        mem=target,
                        cell=ring("cell", part - 1),
                    )
                )
    shares[member, 1] = sums[member, 1]
    for copy in copies:
        copy.wait()
    final = shares[0, 0]
    for m in range(sharers):
        for part in range(3):
            if m or part:
                final = final + shares[m, part]
    out_ref[...] = final


def unpack_kernel(everyone, final_ref, cov_ref, proj_ref):
    width = final_ref.shape[1] // 2
    half = final_ref.shape[0] // REG_DEV
    members = 2 * half
    final = final_ref[...].reshape(half, REG_DEV, 2 * width)
    cov_ref[:half] = final[:, :, :everyone]
    cov_ref[half:] = final[:, :, width : width + everyone]
    lanes = lax.broadcasted_iota(i32, (REG_DEV, members), 1)
    proj = jnp.zeros((REG_DEV, members), f32)
    for m in range(members):
        at = everyone + m // half * width
        proj = jnp.where(lanes == m, final[m % half, :, at : at + 1], proj)
    proj_ref[...] = proj


def on_device(
    state,
    vertical_weight,
    horizontal_weight,
    obs_slot,
    request_cell,
    obs_value,
    obs_error,
    obs_region,
):
    sharers = lax.axis_size("mem")
    cell_dev, members, levels = state.shape
    obs_dev, neigh = obs_slot.shape
    own = obs_dev // TILE
    halo = 3 * obs_dev // 4 // TILE
    far = len(MOVES)
    chunks = own + far * halo
    sources = 1 + far
    buckets = cell_dev // TILE
    steps = chunks + 3 * (buckets - 1)
    share = obs_dev // sharers
    everyone = sharers * members
    width = everyone + 1 + (-(everyone + 1)) % 16
    rows = members // 2 * REG_DEV
    dma = lambda n: pltpu.SemaphoreType.DMA((n,))
    final = pl.pallas_call(
        functools.partial(kernel, own, halo),
        out_shape=jax.ShapeDtypeStruct((rows, 2 * width), f32),
        in_specs=[HBM] * 8,
        out_specs=VMEM,
        scratch_shapes=[
            pltpu.VMEM((chunks, 1, TILE), i32),
            pltpu.VMEM((neigh, obs_dev), i32),
            pltpu.VMEM((neigh, obs_dev), f32),
            pltpu.VMEM((levels, sources * obs_dev), bf16),
            pltpu.VMEM((members * levels, cell_dev), bf16),
            pltpu.VMEM((1, obs_dev), f32),
            pltpu.VMEM((1, obs_dev), f32),
            pltpu.VMEM((1, obs_dev), i32),
            pltpu.VMEM((chunks, 1, TILE), i32),
            pltpu.VMEM((2, chunks, 1, TILE), f32),
            pltpu.VMEM((2, chunks, 1, TILE), f32),
            pltpu.VMEM((6 * chunks, TILE), f32),
            pltpu.VMEM((chunks, levels, TILE), f32),
            pltpu.VMEM((steps, 16, TILE), f32),
            pltpu.VMEM((sources, sharers, members * share // 128, 128), f32),
            pltpu.VMEM((sources, sharers, members * share // 128, 128), f32),
            pltpu.VMEM((sharers, 3, rows, 2 * width), f32),
            pltpu.VMEM((sharers, 3, rows, 2 * width), f32),
            dma(8),
            dma(5),
            dma(5),
            dma(5),
            dma(5),
            dma(sharers),
            dma(sharers),
            dma(5),
            dma(5),
            dma(sources * sharers),
            dma(sources * sharers),
            dma(3 * sharers),
            dma(3 * sharers),
        ],
        compiler_params=pltpu.CompilerParams(
            collective_id=0, has_side_effects=True, vmem_limit_bytes=60 * 2**20
        ),
    )(
        request_cell.reshape(chunks, 1, TILE),
        obs_slot.T,
        horizontal_weight.T,
        vertical_weight.T,
        state.transpose(1, 2, 0).reshape(members * levels, cell_dev),
        obs_value.reshape(1, obs_dev),
        obs_error.reshape(1, obs_dev),
        obs_region.reshape(1, obs_dev),
    )
    cov, proj = pl.pallas_call(
        functools.partial(unpack_kernel, everyone),
        out_shape=(
            jax.ShapeDtypeStruct((members, REG_DEV, everyone), f32),
            jax.ShapeDtypeStruct((REG_DEV, members), f32),
        ),
        in_specs=[VMEM],
        out_specs=(VMEM, VMEM),
    )(final)
    return cov.transpose(1, 0, 2), proj


def solution(mesh):
    in_specs = (
        P("cell", "mem", None),
        P("cell", None),
        P("cell", None),
        P("cell", None),
        P("cell", None),
        P("cell"),
        P("cell"),
        P("cell"),
    )
    out_specs = (P("cell", "mem", None), P("cell", "mem"))
    return jax.shard_map(
        on_device, mesh=mesh, in_specs=in_specs, out_specs=out_specs, check_vma=False
    )
```
